32 devices in a mesh: dp: 2 (over x), tp: 4 (over z), ep: 4 (over y, core).
Axes of the slice: x: 2, y: 2, z: 4, core: 2. Of those that a mesh axis runs over, the one named last changes fastest.
Arguments:
- emb: bfloat16 [2, 512, 2048], P(None, ('dp', 'ep')), parts along dimension 1
- pos: int32 [512], P(('dp', 'ep')), parts along dimension 0
- route_ids: int32 [2, 512, 6], P(None, ('dp', 'ep')), parts along dimension 1
- lat_cache: bfloat16 [2, 512, 64, 512], P(None, ('dp', 'ep')), parts along dimension 1
- rope_cache: bfloat16 [2, 512, 64, 64], P(None, ('dp', 'ep')), parts along dimension 1
- attn_norm: float32 [2, 2048], replicated
- w_q: bfloat16 [2, 2048, 16, 192], P(None, None, 'tp')
- w_dkv: bfloat16 [2, 2048, 576], replicated
- kv_norm: float32 [2, 512], replicated
- w_uk: bfloat16 [2, 512, 16, 128], P(None, None, 'tp')
- w_uv: bfloat16 [2, 512, 16, 128], P(None, None, 'tp')
- w_o: bfloat16 [2, 2048, 2048], P(None, 'tp')
- mlp_norm: float32 [2, 2048], replicated
- dense_gate: bfloat16 [2048, 10944], P(None, 'tp')
- dense_up: bfloat16 [2048, 10944], P(None, 'tp')
- dense_down: bfloat16 [10944, 2048], P('tp')
- router: bfloat16 [2048, 64], replicated
- shared_gate: bfloat16 [2048, 2816], P(None, 'tp')
- shared_up: bfloat16 [2048, 2816], P(None, 'tp')
- shared_down: bfloat16 [2816, 2048], P('tp')
- expert_gate: bfloat16 [64, 2048, 1408], P('ep', None, 'tp')
- expert_up: bfloat16 [64, 2048, 1408], P('ep', None, 'tp')
- expert_down: bfloat16 [64, 1408, 2048], P('ep', 'tp')
Outputs:
- output 1: bfloat16 [2, 512, 2048], P(None, ('dp', 'ep')), parts along dimension 1
- output 2: bfloat16 [2, 512, 64, 512], P(None, ('dp', 'ep')), parts along dimension 1
- output 3: bfloat16 [2, 512, 64, 64], P(None, ('dp', 'ep')), parts along dimension 1
There are 2 independent parts. The reference program is written for one: setup_inputs(seed, part) draws one part's arguments, and reference() takes and returns one part's arrays. A program takes and returns all parts, laid end to end along the dimension named above; an argument that names none is the same for every part.
All inputs are finite; a program needn't handle non-finite values.
Results may differ from the reference program's by a relative error of at most 0.02.
Values are sent between devices in bfloat16 or wider.
A program may use at most 1 GiB of HBM per device.

```python
import math
import jax
import jax.numpy as jnp
from jax import lax

HIDDEN = 2048
NUM_HEADS = 16
NOPE_DIM = 128
ROPE_DIM = 64
KV_LORA = 512
V_HEAD = 128
DENSE_FF = 10944
EXPERTS = 64
EXPERT_FF = 1408
SHARED_FF = 2816
TOP_K = 6
TOKENS = 256
CACHE_LEN = 64

QK_DIM = NOPE_DIM + ROPE_DIM
SCORE_SCALE = 1.0 / math.sqrt(QK_DIM)
NORM_EPS = 1e-6
ROPE_THETA = 10000.0
ROUTE_SCALE = 1.5 * EXPERTS / TOP_K
LATENT_GAIN = 0.5 * math.log(CACHE_LEN)


def rms_norm(values, gain):
    wide = values.astype(jnp.float32)
    mean_sq = jnp.mean(wide * wide, axis=-1, keepdims=True)
    return (wide * lax.rsqrt(mean_sq + NORM_EPS) * gain).astype(jnp.bfloat16)


def rope_tables(position):
    half_dim = ROPE_DIM // 2
    inv_freq = ROPE_THETA ** (-(jnp.arange(half_dim, dtype=jnp.float32) * 2.0 / ROPE_DIM))
    angles = position.astype(jnp.float32)[:, None] * inv_freq[None, :]
    return jnp.cos(angles), jnp.sin(angles)


def rotary(values, cos_t, sin_t):
    wide = values.astype(jnp.float32)
    half_dim = wide.shape[-1] // 2
    first = wide[..., :half_dim]
    second = wide[..., half_dim:]
    return jnp.concatenate([first * cos_t - second * sin_t, second * cos_t + first * sin_t], axis=-1)


def attention(hidden, cur_pos, lat, rop, g_attn, w_query, w_dkv, g_kv, w_uk, w_uv, w_out):
    tokens = hidden.shape[0]
    cos_t, sin_t = rope_tables(cur_pos)
    normed = rms_norm(hidden, g_attn)
    query = jnp.dot(normed, w_query.reshape(HIDDEN, NUM_HEADS * QK_DIM), preferred_element_type=jnp.float32).reshape(tokens, NUM_HEADS, QK_DIM)
    q_nope = query[..., :NOPE_DIM].astype(jnp.bfloat16)
    q_rope = rotary(query[..., NOPE_DIM:], cos_t[:, None, :], sin_t[:, None, :]).astype(jnp.bfloat16)
    kv_proj = jnp.dot(normed, w_dkv, preferred_element_type=jnp.float32)
    lat_new = rms_norm(kv_proj[:, :KV_LORA], g_kv)
    rope_new = rotary(kv_proj[:, KV_LORA:], cos_t, sin_t).astype(jnp.bfloat16)
    slot_ids = jnp.arange(CACHE_LEN)
    hit_mask = (slot_ids[None, :] == cur_pos[:, None])[:, :, None]
    lat = jnp.where(hit_mask, lat_new[:, None, :], lat)
    rop = jnp.where(hit_mask, rope_new[:, None, :], rop)
    q_lat = jnp.einsum('bhn,chn->bhc', q_nope.astype(jnp.float32), w_uk.astype(jnp.float32)).astype(jnp.bfloat16)
    lat_wide = lat.astype(jnp.float32)
    scores = (jnp.einsum('bhc,btc->bht', q_lat.astype(jnp.float32), lat_wide) + jnp.einsum('bhr,btr->bht', q_rope.astype(jnp.float32), rop.astype(jnp.float32))) * SCORE_SCALE
    visible = slot_ids[None, None, :] <= cur_pos[:, None, None]
    scores = jnp.where(visible, scores, -1e30)
    prob_bf = jax.nn.softmax(scores, axis=-1).astype(jnp.bfloat16)
    o_lat = jnp.einsum('bht,btc->bhc', prob_bf.astype(jnp.float32), lat_wide).astype(jnp.bfloat16)
    heads_out = jnp.einsum('bhc,chv->bhv', o_lat.astype(jnp.float32), w_uv.astype(jnp.float32)).astype(jnp.bfloat16)
    attn_sum = jnp.dot(heads_out.reshape(tokens, NUM_HEADS * V_HEAD), w_out, preferred_element_type=jnp.float32)
    return (hidden.astype(jnp.float32) + attn_sum).astype(jnp.bfloat16), lat, rop


def swiglu(normed, w_gate, w_up, w_down):
    gate_h = jnp.dot(normed, w_gate, preferred_element_type=jnp.float32)
    up_h = jnp.dot(normed, w_up, preferred_element_type=jnp.float32)
    act_bf = (jax.nn.silu(gate_h) * up_h).astype(jnp.bfloat16)
    return jnp.dot(act_bf, w_down, preferred_element_type=jnp.float32)


def routed(normed, expert_ids, router, expert_gate, expert_up, expert_down):
    logits = jnp.dot(normed, router, preferred_element_type=jnp.float32)
    probs_all = jax.nn.softmax(logits, axis=-1)
    route_w = jnp.take_along_axis(probs_all, expert_ids, axis=1)
    combine = jnp.sum(route_w[:, :, None] * (expert_ids[:, :, None] == jnp.arange(EXPERTS)[None, None, :]), axis=1)

    def expert_step(total, packed):
        gate_w, up_w, down_w, weight_col = packed
        return total + weight_col[:, None] * swiglu(normed, gate_w, up_w, down_w), None

    start_sum = jnp.zeros((normed.shape[0], HIDDEN), jnp.float32)
    return lax.scan(expert_step, start_sum, (expert_gate, expert_up, expert_down, combine.T))[0]


def setup_inputs(seed: int = 0, part: int = 0) -> dict:
    base = jax.random.key(seed)
    part_keys = jax.random.split(jax.random.fold_in(base, part), 8)
    weight_keys = jax.random.split(jax.random.fold_in(base, 100003), 18)

    def normal(key, shape):
        return jax.random.normal(key, shape, jnp.float32)

    emb = normal(part_keys[0], (2, TOKENS, HIDDEN)).astype(jnp.bfloat16)
    pos = jax.random.randint(part_keys[1], (TOKENS,), 1, CACHE_LEN - 1, dtype=jnp.int32).at[0].set(CACHE_LEN - 2)
    hot_bias = jax.random.randint(part_keys[2], (EXPERTS,), 0, 3, dtype=jnp.int32) * 64
    raw_score = jax.random.randint(part_keys[3], (2, TOKENS, EXPERTS), 0, 128, dtype=jnp.int32) + hot_bias
    keyed = raw_score * EXPERTS + jnp.arange(EXPERTS, dtype=jnp.int32)
    route_ids = lax.top_k(keyed, TOP_K)[1].astype(jnp.int32)
    lat_cache = (0.5 * normal(part_keys[4], (2, TOKENS, 1, KV_LORA)) + 0.2 * normal(part_keys[5], (2, TOKENS, CACHE_LEN, KV_LORA))).astype(jnp.bfloat16)
    rope_cache = (1.5 * normal(part_keys[6], (2, TOKENS, 1, ROPE_DIM)) + 0.3 * normal(part_keys[7], (2, TOKENS, CACHE_LEN, ROPE_DIM))).astype(jnp.bfloat16)
    q_scale = jnp.where(jnp.arange(QK_DIM) < NOPE_DIM, 1.0, 2.0) * HIDDEN ** -0.5
    return dict(
        emb=emb,
        pos=pos,
        route_ids=route_ids,
        lat_cache=lat_cache,
        rope_cache=rope_cache,
        attn_norm=1.0 + 0.25 * normal(weight_keys[0], (2, HIDDEN)),
        w_q=(normal(weight_keys[1], (2, HIDDEN, NUM_HEADS, QK_DIM)) * q_scale).astype(jnp.bfloat16),
        w_dkv=(normal(weight_keys[2], (2, HIDDEN, KV_LORA + ROPE_DIM)) * HIDDEN ** -0.5).astype(jnp.bfloat16),
        kv_norm=1.0 + 0.25 * normal(weight_keys[3], (2, KV_LORA)),
        w_uk=(normal(weight_keys[4], (2, KV_LORA, NUM_HEADS, NOPE_DIM)) * (LATENT_GAIN * NOPE_DIM ** -0.5)).astype(jnp.bfloat16),
        w_uv=(normal(weight_keys[5], (2, KV_LORA, NUM_HEADS, V_HEAD)) * KV_LORA ** -0.5).astype(jnp.bfloat16),
        w_o=(normal(weight_keys[6], (2, NUM_HEADS * V_HEAD, HIDDEN)) * (NUM_HEADS * V_HEAD) ** -0.5).astype(jnp.bfloat16),
        mlp_norm=1.0 + 0.25 * normal(weight_keys[7], (2, HIDDEN)),
        dense_gate=(normal(weight_keys[8], (HIDDEN, DENSE_FF)) * HIDDEN ** -0.5).astype(jnp.bfloat16),
        dense_up=(normal(weight_keys[9], (HIDDEN, DENSE_FF)) * HIDDEN ** -0.5).astype(jnp.bfloat16),
        dense_down=(normal(weight_keys[10], (DENSE_FF, HIDDEN)) * DENSE_FF ** -0.5).astype(jnp.bfloat16),
        router=(normal(weight_keys[11], (HIDDEN, EXPERTS)) * (1.5 * HIDDEN ** -0.5)).astype(jnp.bfloat16),
        shared_gate=(normal(weight_keys[12], (HIDDEN, SHARED_FF)) * HIDDEN ** -0.5).astype(jnp.bfloat16),
        shared_up=(normal(weight_keys[13], (HIDDEN, SHARED_FF)) * HIDDEN ** -0.5).astype(jnp.bfloat16),
        shared_down=(normal(weight_keys[14], (SHARED_FF, HIDDEN)) * SHARED_FF ** -0.5).astype(jnp.bfloat16),
        expert_gate=(normal(weight_keys[15], (EXPERTS, HIDDEN, EXPERT_FF)) * HIDDEN ** -0.5).astype(jnp.bfloat16),
        expert_up=(normal(weight_keys[16], (EXPERTS, HIDDEN, EXPERT_FF)) * HIDDEN ** -0.5).astype(jnp.bfloat16),
        expert_down=(normal(weight_keys[17], (EXPERTS, EXPERT_FF, HIDDEN)) * (ROUTE_SCALE * EXPERT_FF ** -0.5)).astype(jnp.bfloat16),
    )


def reference(emb, pos, route_ids, lat_cache, rope_cache, attn_norm, w_q, w_dkv, kv_norm, w_uk, w_uv, w_o, mlp_norm, dense_gate, dense_up, dense_down, router, shared_gate, shared_up, shared_down, expert_gate, expert_up, expert_down):
    lat_first, lat_second = lat_cache[0], lat_cache[1]
    rop_first, rop_second = rope_cache[0], rope_cache[1]
    hidden_steps = []
    for step_idx in range(2):
        cur_pos = pos + step_idx
        y_first, lat_first, rop_first = attention(emb[step_idx], cur_pos, lat_first, rop_first, attn_norm[0], w_q[0], w_dkv[0], kv_norm[0], w_uk[0], w_uv[0], w_o[0])
        dense_out = swiglu(rms_norm(y_first, mlp_norm[0]), dense_gate, dense_up, dense_down)
        h_mid = (y_first.astype(jnp.float32) + dense_out).astype(jnp.bfloat16)
        y_second, lat_second, rop_second = attention(h_mid, cur_pos, lat_second, rop_second, attn_norm[1], w_q[1], w_dkv[1], kv_norm[1], w_uk[1], w_uv[1], w_o[1])
        normed = rms_norm(y_second, mlp_norm[1])
        moe_out = swiglu(normed, shared_gate, shared_up, shared_down) + routed(normed, route_ids[step_idx], router, expert_gate, expert_up, expert_down)
        hidden_steps.append((y_second.astype(jnp.float32) + moe_out).astype(jnp.bfloat16))
    return jnp.stack(hidden_steps), jnp.stack([lat_first, lat_second]), jnp.stack([rop_first, rop_second])
```

```python
import functools
import math
import jax
import jax.numpy as jnp
from jax import lax
from jax.experimental import pallas as pl
from jax.experimental.pallas import tpu as pltpu
from jax.sharding import PartitionSpec as P

NORM_EPS = 1e-6
ROPE_THETA = 10000.0
MESH = pl.DeviceIdType.MESH
VMEM = pltpu.VMEM
DMA = pltpu.SemaphoreType.DMA
VMEM_CAP = 62 * 1024 * 1024
SEQ_BLOCK = 8
CHUNKS = 4
LAGS = (1, 4, 5, 6, 8)
COMBINE_CHUNKS = 8
COMBINE_LAGS = (1, 3, 5, 6, 9)
ROW_TILE = 128


def rms_norm(values, gain):
    wide = values.astype(jnp.float32)
    mean_sq = jnp.mean(wide * wide, axis=-1, keepdims=True)
    return (wide * lax.rsqrt(mean_sq + NORM_EPS) * gain).astype(jnp.bfloat16)


def rope_tables(position, rope_dim):
    half_dim = rope_dim // 2
    inv_freq = ROPE_THETA ** (-(jnp.arange(half_dim, dtype=jnp.float32) * 2.0 / rope_dim))
    angles = position.astype(jnp.float32)[:, None] * inv_freq[None, :]
    return jnp.cos(angles), jnp.sin(angles)


def rotary(values, cos_t, sin_t):
    wide = values.astype(jnp.float32)
    half_dim = wide.shape[-1] // 2
    first = wide[..., :half_dim]
    second = wide[..., half_dim:]
    return jnp.concatenate([first * cos_t - second * sin_t, second * cos_t + first * sin_t], axis=-1)


def fdot(a, b):
    return jnp.dot(a, b, preferred_element_type=jnp.float32)


def attn_kernel(scale, heads, pos_smem, q_lat, q_pe, lat_new, rope_new, lat_in, rope_in, *rest):
    lat_out, rope_out, o_ref = rest[-3:]
    base = pl.program_id(0) * SEQ_BLOCK
    slots = lat_in.shape[2]
    row_l = lax.broadcasted_iota(jnp.int32, (slots, lat_in.shape[3]), 0)
    row_r = lax.broadcasted_iota(jnp.int32, (slots, rope_in.shape[3]), 0)
    queries = q_lat.shape[1]
    step = (lax.broadcasted_iota(jnp.int32, (queries, slots), 0) >= heads).astype(jnp.int32)
    slot = lax.broadcasted_iota(jnp.int32, (queries, slots), 1)
    nt = (((1,), (1,)), ((), ()))
    for i in range(SEQ_BLOCK):
        p = pos_smem[base + i]
        lat = lat_in[0, i].astype(jnp.float32)
        rop = rope_in[0, i].astype(jnp.float32)
        for s in range(2):
            lat = jnp.where(row_l == p + s, lat_new[i, s:s + 1, :].astype(jnp.float32), lat)
            rop = jnp.where(row_r == p + s, rope_new[i, s:s + 1, :].astype(jnp.float32), rop)
        lat = lat.astype(jnp.bfloat16)
        rop = rop.astype(jnp.bfloat16)
        lat_out[0, i] = lat
        rope_out[0, i] = rop
        sc = lax.dot_general(q_lat[i], lat, nt, preferred_element_type=jnp.float32)
        sc = (sc + lax.dot_general(q_pe[i], rop, nt, preferred_element_type=jnp.float32)) * scale
        sc = jnp.where(slot <= p + step, sc, -1e30)
        e = jnp.exp(sc - jnp.max(sc, axis=-1, keepdims=True))
        prob = (e / jnp.sum(e, axis=-1, keepdims=True)).astype(jnp.bfloat16)
        o_ref[i] = fdot(prob, lat).astype(jnp.bfloat16)


def attn_core(layer, scale, heads, pos, q_lat, q_pe, lat_new, rope_new, lat_cache, rope_cache, prev):
    _, seqs, slots, width = lat_cache.shape
    rope = rope_cache.shape[3]
    queries = q_lat.shape[1]
    blk = lambda *tail: pl.BlockSpec((SEQ_BLOCK,) + tail, lambda i: (i, 0, 0))
    lay = lambda *tail: pl.BlockSpec((1, SEQ_BLOCK) + tail, lambda i: (layer, i, 0, 0))
    in_specs = [pl.BlockSpec(memory_space=pltpu.SMEM), blk(queries, width), blk(queries, rope), blk(2, width), blk(2, rope), lay(slots, width), lay(slots, rope)]
    args = [pos, q_lat, q_pe, lat_new, rope_new, lat_cache, rope_cache]
    alias = {}
    if prev is not None:
        in_specs += [pl.BlockSpec(memory_space=pl.ANY)] * 2
        args += list(prev)
        alias = {7: 0, 8: 1}
    return pl.pallas_call(
        functools.partial(attn_kernel, scale, heads),
        grid=(seqs // SEQ_BLOCK,),
        out_shape=(jax.ShapeDtypeStruct(lat_cache.shape, jnp.bfloat16), jax.ShapeDtypeStruct(rope_cache.shape, jnp.bfloat16), jax.ShapeDtypeStruct(q_lat.shape, jnp.bfloat16)),
        in_specs=in_specs,
        out_specs=(lay(slots, width), lay(slots, rope), blk(queries, width)),
        input_output_aliases=alias,
        compiler_params=pltpu.CompilerParams(dimension_semantics=("arbitrary",), vmem_limit_bytes=32 * 1024 * 1024),
        name=f"attn{layer}",
    )(*args)


def barrier(z, ends, extra):
    sem = pltpu.get_barrier_semaphore()

    @pl.when(z > 0)
    def _():
        pl.semaphore_signal(sem, inc=1, device_id={"tp": z - 1}, device_id_type=MESH)

    @pl.when(z < ends)
    def _():
        pl.semaphore_signal(sem, inc=1, device_id={"tp": z + 1}, device_id_type=MESH)

    for dev in extra:
        pl.semaphore_signal(sem, inc=1, device_id=dev, device_id_type=MESH)
    count = len(extra) + jnp.where(z > 0, 1, 0) + jnp.where(z < ends, 1, 0)
    pl.semaphore_wait(sem, count)


class Line:
    def __init__(self, z, ends, chunks, src, buf, out, residual, sems):
        self.z, self.ends, self.chunks = z, ends, chunks
        self.src, self.buf, self.out, self.residual = src, buf, out, residual
        self.rs_s, self.rs_r, self.bc_s, self.bc_r = sems
        self.rows = src.shape[0] // (2 * chunks)
        low = 2 * z < ends
        self.near = jnp.where(low, 1, 0)
        self.far = 1 - self.near
        self.near_at = jnp.where(low, z, ends - z)
        self.far_at = ends - self.near_at
        up, down = jnp.minimum(z + 1, ends), jnp.maximum(z - 1, 0)
        self.inward = jnp.where(low, up, down)
        self.outward = jnp.where(low, down, up)

    def sl(self, d, c):
        return pl.ds(pl.multiple_of((d * self.chunks + c) * self.rows, self.rows), self.rows)

    def rs(self, d, c, src, dev):
        return pltpu.make_async_remote_copy(src_ref=src, dst_ref=self.buf.at[d, c], send_sem=self.rs_s.at[d, c], recv_sem=self.rs_r.at[d, c], device_id={"tp": dev}, device_id_type=MESH)

    def bc(self, d, c, dev):
        ref = self.out.at[self.sl(d, c)]
        return pltpu.make_async_remote_copy(src_ref=ref, dst_ref=ref, send_sem=self.bc_s.at[d, c], recv_sem=self.bc_r.at[d, c], device_id={"tp": dev}, device_id_type=MESH)

    def reduce_near(self, c):
        d, sl, src, buf = self.near, self.sl(self.near, c), self.src, self.buf

        @pl.when(self.near_at == 0)
        def _():
            self.rs(d, c, src.at[sl], self.inward).start()

        @pl.when(self.near_at > 0)
        def _():
            self.rs(d, c, src.at[sl], self.inward).wait_recv()
            buf[d, c] = buf[d, c] + src[sl]
            self.rs(d, c, buf.at[d, c], self.inward).start()

    def reduce_far(self, c):
        d, sl, src, buf = self.far, self.sl(self.far, c), self.src, self.buf

        @pl.when(self.near_at > 0)
        def _():
            self.rs(d, c, src.at[sl], self.outward).wait_recv()
            buf[d, c] = buf[d, c] + src[sl]
            self.rs(d, c, buf.at[d, c], self.outward).start()

    def finish_far(self, c):
        d, sl, src, buf = self.far, self.sl(self.far, c), self.src, self.buf

        @pl.when(self.near_at == 0)
        def _():
            self.rs(d, c, src.at[sl], self.outward).wait_recv()
            self.out[sl] = (self.residual[sl].astype(jnp.float32) + (buf[d, c] + src[sl])).astype(jnp.bfloat16)
            self.bc(d, c, self.inward).start()

    def spread_far(self, c):
        @pl.when(self.near_at > 0)
        def _():
            self.bc(self.far, c, self.inward).wait_recv()
            self.bc(self.far, c, self.inward).start()

    def spread_near(self, c):
        @pl.when(self.near_at > 0)
        def _():
            self.bc(self.near, c, self.outward).wait_recv()
            self.bc(self.near, c, self.outward).start()

    def finish_near(self, c):
        @pl.when(self.near_at == 0)
        def _():
            self.bc(self.near, c, self.outward).wait_recv()

    def drain(self, c):
        self.rs(self.near, c, self.src.at[self.sl(self.near, c)], self.inward).wait_send()
        self.bc(self.far, c, self.inward).wait_send()

        @pl.when(self.near_at > 0)
        def _():
            self.rs(self.far, c, self.src.at[self.sl(self.far, c)], self.outward).wait_send()
            self.bc(self.near, c, self.outward).wait_send()

    def stage(self, t, lags=LAGS):
        for fn, lag in ((self.reduce_near, 0), (self.reduce_far, lags[0]), (self.finish_far, lags[1]), (self.spread_far, lags[2]), (self.spread_near, lags[3]), (self.finish_near, lags[4])):
            if 0 <= t - lag < self.chunks:
                fn(t - lag)

    def run(self):
        for t in range(self.chunks + max(LAGS)):
            self.stage(t)
        for c in range(self.chunks):
            self.drain(c)


def line_scratch(rows, tail, chunks=CHUNKS):
    return [VMEM((2, chunks, rows // (2 * chunks)) + tail, jnp.float32)] + [DMA((2, chunks)) for _ in range(4)]


def norm_rows(src, gain, dst, step=32):
    for r in range(0, src.shape[0], step):
        dst[r:r + step, :] = rms_norm(src[r:r + step, :], gain[...])


def fdot_t(a, b):
    return lax.dot_general(a, b, (((1,), (1,)), ((), ())), preferred_element_type=jnp.float32)


def mlp_act(x, gate, up, act, block):
    def body(j, carry):
        js = pl.ds(pl.multiple_of(j * block, 16), block)
        g = fdot_t(gate[js, :], x[...])
        u = fdot_t(up[js, :], x[...])
        act[js, :] = (g * jax.nn.sigmoid(g) * u).astype(jnp.bfloat16)
        return carry

    lax.fori_loop(0, gate.shape[0] // block, body, 0)


def mlp_down(act, down, put):
    def body(j, carry):
        ns = pl.ds(pl.multiple_of(j * 512, 512), 512)
        put(ns, lax.dot_general(act[...], down[:, ns], (((0,), (0,)), ((), ())), preferred_element_type=jnp.float32))
        return carry

    lax.fori_loop(0, down.shape[1] // 512, body, 0)


def load(pairs, sem):
    copies = []
    for k, (src, dst) in enumerate(pairs):
        cp = pltpu.make_async_copy(src, dst, sem.at[k])
        cp.start()
        copies.append(cp)
    return copies


def dense_kernel(part, res, gain, gain_next, ids, w_gate, w_up, w_down, h_out, n_out, ids_out, y, x, gate, up, down, act, part2, id_s, id_r, w_sem, *line):
    z, e = lax.axis_index("tp"), lax.axis_index("ep")
    ends = lax.axis_size("tp") - 1
    width = gate.shape[0]
    loads = load([(w_gate, gate), (w_up, up), (w_down, down)], w_sem)
    n_ep = lax.axis_size("ep")
    peers = [{"ep": lax.rem(e + k, n_ep)} for k in range(1, n_ep)]
    barrier(z, ends, peers)
    sends = []
    for k, dev in enumerate(peers):
        cp = pltpu.make_async_remote_copy(src_ref=ids, dst_ref=ids_out.at[k + 1], send_sem=id_s.at[k], recv_sem=id_r.at[k], device_id=dev, device_id_type=MESH)
        cp.start()
        sends.append(cp)
    ids_out[0] = ids[...]
    one = Line(z, ends, CHUNKS, part, line[0], y, res, line[1:5])
    one.run()
    norm_rows(y, gain, x)
    loads[0].wait()
    loads[1].wait()
    mlp_act(x, gate, up, act, width // 3)
    loads[2].wait()

    def put(ns, v):
        part2[:, ns] = v

    mlp_down(act, down, put)
    two = Line(z, ends, CHUNKS, part2, line[5], h_out, y, line[6:10])
    two.run()
    norm_rows(h_out, gain_next, n_out)
    for cp in sends:
        cp.wait()


def dense_block(part, res, gain, gain_next, ids, w_gate, w_up, w_down):
    rows, hidden = part.shape
    width = w_gate.shape[0]
    vm = pl.BlockSpec(memory_space=VMEM)
    hbm = pl.BlockSpec(memory_space=pl.ANY)
    bf = lambda *s: jax.ShapeDtypeStruct(s, jnp.bfloat16)
    line = line_scratch(rows, (hidden,))
    return pl.pallas_call(
        dense_kernel,
        out_shape=(bf(rows, hidden), bf(rows, hidden), jax.ShapeDtypeStruct((4,) + ids.shape, jnp.int32)),
        in_specs=[vm] * 5 + [hbm] * 3,
        out_specs=(vm, vm, vm),
        scratch_shapes=[VMEM((rows, hidden), jnp.bfloat16), VMEM((rows, hidden), jnp.bfloat16), VMEM((width, hidden), jnp.bfloat16), VMEM((width, hidden), jnp.bfloat16), VMEM((width, hidden), jnp.bfloat16), VMEM((width, rows), jnp.bfloat16), VMEM((rows, hidden), jnp.float32), DMA((3,)), DMA((3,)), DMA((3,))] + line + line,
        compiler_params=pltpu.CompilerParams(collective_id=1, has_side_effects=True, vmem_limit_bytes=VMEM_CAP),
        name="dense",
    )(part, res, gain, gain_next, ids, w_gate, w_up, w_down)


def gather_kernel(part, res, gain, w_gate, w_up, w_down, y, x_all, shared, gate, up, down, act, w_sem, c_s, c_r, y_s, y_r, f_s, f_r, *line):
    z, e = lax.axis_index("tp"), lax.axis_index("ep")
    ends = lax.axis_size("tp") - 1
    width = gate.shape[0]
    rows, hidden = y.shape
    loads = load([(w_gate, gate), (w_up, up), (w_down, down)], w_sem)
    core, chip = jnp.bitwise_xor(e, 1), jnp.bitwise_xor(e, 2)
    barrier(z, ends, [{"ep": core}, {"ep": chip}])
    one = Line(z, ends, CHUNKS, part, line[0], y, res, line[1:5])
    one.run()
    mine = x_all.at[e]
    for r in range(0, rows, 32):
        x_all[e, r:r + 32, :] = rms_norm(y[r:r + 32, :], gain[...])

    def copy(src, dst, ss, rs, dev):
        return pltpu.make_async_remote_copy(src_ref=src, dst_ref=dst, send_sem=ss, recv_sem=rs, device_id={"ep": dev}, device_id_type=MESH)

    half = rows // 4
    to_chip = [copy(x_all.at[e, pl.ds(k * half, half)], x_all.at[e, pl.ds(k * half, half)], y_s.at[k], y_r.at[k], chip) for k in range(4)]
    for cp in to_chip:
        cp.start()
    to_core = copy(mine, mine, c_s, c_r, core)
    to_core.start()
    loads[0].wait()
    loads[1].wait()
    mlp_act(mine, gate, up, act, width // 2)
    loads[2].wait()

    def put(ns, v):
        for j in range(4):
            shared[:, ns.start // 128 + j, :] = v[:, j * 128:(j + 1) * 128]

    mlp_down(act, down, put)
    fwd = []
    for k in range(4):
        to_chip[k].wait_recv()
        ref = x_all.at[chip, pl.ds(k * half, half)]
        cp = copy(ref, ref, f_s.at[k], f_r.at[k], core)
        cp.start()
        fwd.append(cp)
    for k in range(4):
        to_chip[k].wait_send()
        fwd[k].wait()
    to_core.wait()


def gather_block(part, res, gain, w_gate, w_up, w_down):
    rows, hidden = part.shape
    width = w_gate.shape[0]
    vm = pl.BlockSpec(memory_space=VMEM)
    hbm = pl.BlockSpec(memory_space=pl.ANY)
    return pl.pallas_call(
        gather_kernel,
        out_shape=(jax.ShapeDtypeStruct((rows, hidden), jnp.bfloat16), jax.ShapeDtypeStruct((4, rows, hidden), jnp.bfloat16), jax.ShapeDtypeStruct((rows, hidden // 128, 128), jnp.float32)),
        in_specs=[vm] * 3 + [hbm] * 3,
        out_specs=(vm, vm, vm),
        scratch_shapes=[VMEM((width, hidden), jnp.bfloat16), VMEM((width, hidden), jnp.bfloat16), VMEM((width, hidden), jnp.bfloat16), VMEM((width, rows), jnp.bfloat16), DMA((3,)), DMA, DMA, DMA((4,)), DMA((4,)), DMA((4,)), DMA((4,))] + line_scratch(rows, (hidden,)),
        compiler_params=pltpu.CompilerParams(collective_id=2, has_side_effects=True, vmem_limit_bytes=VMEM_CAP),
        name="gather",
    )(part, res, gain, w_gate, w_up, w_down)


def expert_kernel(own, counts, lists, weights, x_all, shared, w_gate, w_up, w_down, acc, acc_s, x3, rows3, xb, d3):
    e = pl.program_id(0)
    tokens, slabs = x3.shape[0], x3.shape[1]
    local = pl.num_programs(0)

    @pl.when(e == 0)
    def _():
        acc_s[...] = jnp.zeros_like(acc_s)
        rows3[...] = jnp.zeros_like(rows3)
        acc_s[pl.ds(own[0] * shared.shape[0], shared.shape[0])] = shared[...]

        def widen(i, carry):
            r = pl.ds(pl.multiple_of(i * 64, 64), 64)
            for k in range(slabs):
                x3[r, k, :] = x_all[r, k * 128:(k + 1) * 128].astype(jnp.float32)
            return carry

        lax.fori_loop(0, tokens // 64, widen, 0)

    n = counts[e]

    def tile(i, carry):
        first = e * tokens + i * ROW_TILE
        left = jnp.minimum(n - i * ROW_TILE, ROW_TILE)
        groups = (left + 7) // 8

        def fetch(g, c):
            for r in range(8):
                rows3[g * 8 + r] = x3[lists[first + g * 8 + r]]
            return c

        lax.fori_loop(0, groups, fetch, 0)
        half = ROW_TILE // 2

        def pack(lo):
            for k in range(slabs):
                xb[lo:lo + half, k * 128:(k + 1) * 128] = rows3[lo:lo + half, k, :].astype(jnp.bfloat16)

        pack(0)
        pl.when(left > half)(lambda: pack(half))
        g = fdot_t(w_gate[0], xb[...])
        u = fdot_t(w_up[0], xb[...])
        act = (g * jax.nn.sigmoid(g) * u).astype(jnp.bfloat16)
        for c in range(0, slabs, 4):
            d = lax.dot_general(act, w_down[0, :, c * 128:(c + 4) * 128], (((0,), (0,)), ((), ())), preferred_element_type=jnp.float32)
            for k in range(4):
                d3[:, c + k, :] = d[:, k * 128:(k + 1) * 128]

        def scatter(g, c):
            ts = []
            for r in range(8):
                ok = g * 8 + r < left
                ts.append(jnp.where(ok, lists[first + g * 8 + r], tokens))
            vals = [acc_s[ts[r]] + weights[jnp.minimum(ts[r], tokens - 1) * local + e] * d3[g * 8 + r] for r in range(8)]
            for r in range(8):
                acc_s[ts[r]] = vals[r]
            return c

        lax.fori_loop(0, groups, scatter, 0)
        return carry

    lax.fori_loop(0, (n + ROW_TILE - 1) // ROW_TILE, tile, 0)

    @pl.when(e == local - 1)
    def _():
        acc[...] = acc_s[pl.ds(0, tokens)]


def expert_block(own, counts, lists, weights, x_all, shared, w_gate, w_up, w_down):
    tokens, hidden = x_all.shape
    local, width, _ = w_gate.shape
    slabs = hidden // 128
    sm = pl.BlockSpec(memory_space=pltpu.SMEM)
    vm = pl.BlockSpec(memory_space=VMEM)
    return pl.pallas_call(
        expert_kernel,
        grid=(local,),
        out_shape=jax.ShapeDtypeStruct((tokens, slabs, 128), jnp.float32),
        in_specs=[sm, sm, sm, sm, vm, vm, pl.BlockSpec((1, width, hidden), lambda e: (e, 0, 0)), pl.BlockSpec((1, width, hidden), lambda e: (e, 0, 0)), pl.BlockSpec((1, width, hidden), lambda e: (e, 0, 0))],
        out_specs=vm,
        scratch_shapes=[VMEM((tokens + 8, slabs, 128), jnp.float32), VMEM((tokens, slabs, 128), jnp.float32), VMEM((ROW_TILE, slabs, 128), jnp.float32), VMEM((ROW_TILE, hidden), jnp.bfloat16), VMEM((ROW_TILE, slabs, 128), jnp.float32)],
        compiler_params=pltpu.CompilerParams(dimension_semantics=("arbitrary",), vmem_limit_bytes=VMEM_CAP),
        name="experts",
    )(own, counts, lists, weights, x_all, shared, w_gate, w_up, w_down)


def combine_kernel(acc, res, out, total, from_core, from_chip, own_sum, c_s, c_r, y_s, y_r, *line):
    z, e = lax.axis_index("tp"), lax.axis_index("ep")
    ends = lax.axis_size("tp") - 1
    core, chip = jnp.bitwise_xor(e, 1), jnp.bitwise_xor(e, 2)
    both = jnp.bitwise_xor(e, 3)
    barrier(z, ends, [{"ep": core}, {"ep": chip}])
    rows = res.shape[0]
    step = rows // (2 * COMBINE_CHUNKS)
    order = [(d, c) for c in range(COMBINE_CHUNKS) for d in range(2)]

    def copy(src, dst, ss, rs, dev):
        return pltpu.make_async_remote_copy(src_ref=src, dst_ref=dst, send_sem=ss, recv_sem=rs, device_id={"ep": dev}, device_id_type=MESH)

    hops = []
    for w, block in enumerate((both, core)):
        for d, c in order:
            k = d * COMBINE_CHUNKS + c
            cp = copy(acc.at[pl.ds(block * rows + k * step, step)], from_core.at[w, pl.ds(k * step, step)], c_s.at[w, k], c_r.at[w, k], core)
            cp.start()
            hops.append(cp)
    n = len(order)
    outs = []
    for j, (d, c) in enumerate(order):
        k = d * COMBINE_CHUNKS + c
        hops[j].wait_recv()
        sl = pl.ds(k * step, step)
        total[sl] = acc[pl.ds(chip * rows + k * step, step)] + from_core[0, sl]
        cp = copy(total.at[sl], from_chip.at[sl], y_s.at[k], y_r.at[k], chip)
        cp.start()
        outs.append(cp)
    one = Line(z, ends, COMBINE_CHUNKS, own_sum, line[0], out, res, line[1:5])
    for t in range(COMBINE_CHUNKS + max(COMBINE_LAGS)):
        for j in (2 * t, 2 * t + 1):
            if j < n:
                d, c = order[j]
                sl = pl.ds((d * COMBINE_CHUNKS + c) * step, step)
                hops[n + j].wait_recv()
                outs[j].wait_recv()
                own_sum[sl] = (acc[pl.ds(e * rows + (d * COMBINE_CHUNKS + c) * step, step)] + from_core[1, sl]) + from_chip[sl]
        one.stage(t, COMBINE_LAGS)
    for c in range(COMBINE_CHUNKS):
        one.drain(c)
    for cp in hops + outs:
        cp.wait_send()


def combine_block(acc, res):
    rows, slabs, lanes = res.shape
    vm = pl.BlockSpec(memory_space=VMEM)
    f32 = lambda *s: VMEM(s, jnp.float32)
    n = 2 * COMBINE_CHUNKS
    return pl.pallas_call(
        combine_kernel,
        out_shape=jax.ShapeDtypeStruct(res.shape, jnp.bfloat16),
        in_specs=[vm, vm],
        out_specs=vm,
        scratch_shapes=[f32(rows, slabs, lanes), f32(2, rows, slabs, lanes), f32(rows, slabs, lanes), f32(rows, slabs, lanes), DMA((2, n)), DMA((2, n)), DMA((n,)), DMA((n,))] + line_scratch(rows, (slabs, lanes), COMBINE_CHUNKS),
        compiler_params=pltpu.CompilerParams(collective_id=3, has_side_effects=True, vmem_limit_bytes=VMEM_CAP),
        name="combine",
    )(acc, res)


def attention(layer, normed, pos, cos_t, sin_t, lat_cache, rope_cache, prev, w_q, w_dkv, kv_norm, w_uk, w_uv, w_o):
    nope_dim = w_uk.shape[2]
    heads, qk_dim = w_q.shape[1], w_q.shape[2]
    lora = kv_norm.shape[0]
    rows = normed.shape[0]
    seqs = rows // 2
    query = jnp.einsum('bd,dhk->bhk', normed, w_q, preferred_element_type=jnp.float32)
    q_nope = query[..., :nope_dim].astype(jnp.bfloat16)
    q_pe = rotary(query[..., nope_dim:], cos_t[:, None, :], sin_t[:, None, :]).astype(jnp.bfloat16)
    kv = fdot(normed, w_dkv)
    lat_new = rms_norm(kv[:, :lora], kv_norm)
    rope_new = rotary(kv[:, lora:], cos_t, sin_t).astype(jnp.bfloat16)
    q_lat = jnp.einsum('bhn,chn->bhc', q_nope, w_uk, preferred_element_type=jnp.float32).astype(jnp.bfloat16)
    by_seq = lambda v: v.reshape((2, seqs) + v.shape[1:]).swapaxes(0, 1)
    lat, rop, o_lat = attn_core(layer, 1.0 / math.sqrt(qk_dim), heads, pos, by_seq(q_lat).reshape(seqs, 2 * heads, lora), by_seq(q_pe).reshape(seqs, 2 * heads, -1), by_seq(lat_new), by_seq(rope_new), lat_cache, rope_cache, prev)
    o_lat = o_lat.reshape(seqs, 2, heads, lora).swapaxes(0, 1).reshape(rows, heads, lora)
    heads_out = jnp.einsum('bhc,chv->bhv', o_lat, w_uv, preferred_element_type=jnp.float32).astype(jnp.bfloat16)
    return fdot(heads_out.reshape(rows, -1), w_o), (lat, rop)


def token_lists(ids, ep, local):
    tokens = ids.shape[0]
    mine = jnp.any(ids[:, :, None] == (ep * local + jnp.arange(local))[None, None, :], axis=1)
    lower = (jnp.arange(tokens)[:, None] > jnp.arange(tokens)[None, :]).astype(jnp.bfloat16)
    rank = fdot(lower, mine.astype(jnp.bfloat16)).astype(jnp.int32)
    rank = jnp.where(mine, rank, -1)
    hit = rank.T[:, None, :] == jnp.arange(tokens)[None, :, None]
    lists = jnp.sum(jnp.where(hit, jnp.arange(tokens)[None, None, :], 0), axis=2)
    counts = jnp.sum(mine.astype(jnp.int32), axis=0)
    return mine, lists.astype(jnp.int32), counts


def solution(mesh):
    tok_axes = ('dp', 'ep')

    def device_fn(emb, pos, route_ids, lat_cache, rope_cache, attn_norm, w_q, w_dkv, kv_norm, w_uk, w_uv, w_o, mlp_norm, dense_gate, dense_up, dense_down, router, shared_gate, shared_up, shared_down, expert_gate, expert_up, expert_down):
        _, seqs, hidden = emb.shape
        rows = 2 * seqs
        ep = lax.axis_index('ep')
        n_ep = lax.axis_size('ep')
        local = expert_gate.shape[0]
        top_k = route_ids.shape[2]
        cur = jnp.concatenate([pos, pos + 1])
        cos_t, sin_t = rope_tables(cur, rope_cache.shape[-1])
        h0 = emb.reshape(rows, hidden)
        part, caches = attention(0, rms_norm(h0, attn_norm[0]), pos, cos_t, sin_t, lat_cache, rope_cache, None, w_q[0], w_dkv[0], kv_norm[0], w_uk[0], w_uv[0], w_o[0])
        flat = route_ids.reshape(-1)
        ids = jnp.pad(flat, (0, -flat.size % 1024)).reshape(-1, 128)
        h_mid, normed, ids_all = dense_block(part, h0, mlp_norm[0][None], attn_norm[1][None], ids, dense_gate.T, dense_up.T, dense_down)
        ids_all = ids_all[jnp.mod(ep - jnp.arange(n_ep), n_ep)].reshape(n_ep, -1)[:, :flat.size].reshape(n_ep * rows, top_k)
        mine, lists, counts = token_lists(ids_all, ep, local)
        part, caches = attention(1, normed, pos, cos_t, sin_t, lat_cache, rope_cache, caches, w_q[1], w_dkv[1], kv_norm[1], w_uk[1], w_uv[1], w_o[1])
        y, x_all, shared = gather_block(part, h_mid, mlp_norm[1][None], shared_gate.T, shared_up.T, shared_down)
        x_all = x_all.reshape(n_ep * rows, hidden)
        probs = jax.nn.softmax(fdot(x_all, router), axis=-1)
        weights = lax.dynamic_slice_in_dim(probs, ep * local, local, axis=1)
        acc = expert_block(ep.reshape(1), counts, lists.reshape(-1), weights.reshape(-1), x_all, shared, expert_gate.swapaxes(1, 2), expert_up.swapaxes(1, 2), expert_down)
        out = combine_block(acc, y.reshape(rows, hidden // 128, 128))
        return out.reshape(2, seqs, hidden), caches[0], caches[1]

    in_specs = (P(None, tok_axes, None), P(tok_axes), P(None, tok_axes, None), P(None, tok_axes, None, None), P(None, tok_axes, None, None), P(), P(None, None, 'tp', None), P(), P(), P(None, None, 'tp', None), P(None, None, 'tp', None), P(None, 'tp', None), P(), P(None, 'tp'), P(None, 'tp'), P('tp', None), P(), P(None, 'tp'), P(None, 'tp'), P('tp', None), P('ep', None, 'tp'), P('ep', None, 'tp'), P('ep', 'tp', None))
    out_specs = (P(None, tok_axes, None), P(None, tok_axes, None, None), P(None, tok_axes, None, None))
    return jax.shard_map(device_fn, mesh=mesh, in_specs=in_specs, out_specs=out_specs, check_vma=False)
```

```python
import functools
import math
import jax
import jax.numpy as jnp
from jax import lax
from jax.experimental import pallas as pl
from jax.experimental.pallas import tpu as pltpu
from jax.sharding import PartitionSpec as P

NORM_EPS = 1e-6
ROPE_THETA = 10000.0
MESH = pl.DeviceIdType.MESH
VMEM = pltpu.VMEM
DMA = pltpu.SemaphoreType.DMA
VMEM_CAP = 62 * 1024 * 1024
SEQ_BLOCK = 16
SEQ_GROUP = 8
CHUNKS = 8
LAGS = (2, 8, 7, 9, 18)
COMBINE_CHUNKS = 8
COMBINE_LAGS = (1, 3, 5, 6, 9)
ROW_TILE = 128
GROUP = 16


def rms_norm(values, gain):
    wide = values.astype(jnp.float32)
    mean_sq = jnp.mean(wide * wide, axis=-1, keepdims=True)
    return (wide * lax.rsqrt(mean_sq + NORM_EPS) * gain).astype(jnp.bfloat16)


def rope_tables(position, rope_dim):
    half_dim = rope_dim // 2
    inv_freq = ROPE_THETA ** (-(jnp.arange(half_dim, dtype=jnp.float32) * 2.0 / rope_dim))
    angles = position.astype(jnp.float32)[:, None] * inv_freq[None, :]
    return jnp.cos(angles), jnp.sin(angles)


def fdot(a, b):
    return jnp.dot(a, b, preferred_element_type=jnp.float32)


def rotate_t(v, cos, sin):
    half = v.shape[0] // 2
    first, second = v[:half], v[half:]
    return jnp.concatenate([first * cos - second * sin, second * cos + first * sin], axis=0)


def rounded(v):
    return v.astype(jnp.bfloat16).astype(jnp.float32)


def attn_kernel(layer, scale, pos_smem, h, gain, kv_gain, cos, sin, w_q, w_kv, w_uk, w_uv, w_o, lat_in, rope_in, *rest):
    lat_out, rope_out, part, x, q_s, qp_s, ln_s, rn_s, o_s = rest[-9:]
    step_id = pl.program_id(0)
    heads, qk = w_q.shape[1], w_q.shape[2]
    seqs, queries, lora = q_s.shape
    rope = rope_in.shape[3]
    nope = qk - rope

    @pl.when(step_id == 0)
    def _():
        norm_rows(h, gain.at[layer:layer + 1], x)
        kv = fdot_t(w_kv[0], x[...])
        lat = kv[:lora]
        lat = lat * lax.rsqrt(jnp.mean(lat * lat, axis=0, keepdims=True) + NORM_EPS)
        ln_s[...] = rounded(lat.T * kv_gain[layer:layer + 1, :])
        rn_s[...] = rounded(rotate_t(kv[lora:], cos[...], sin[...])).T
        for n in range(heads):
            q = fdot_t(w_q[0, n], x[...])
            q_nope = q[:nope].T.astype(jnp.bfloat16)
            q_pe = rotate_t(q[nope:], cos[...], sin[...]).T
            q_lat = fdot_t(q_nope, w_uk[0, :, n, :])
            for s in range(2):
                q_s[:, s * heads + n, :] = q_lat[s * seqs:(s + 1) * seqs]
                qp_s[:, s * heads + n, :] = q_pe[s * seqs:(s + 1) * seqs]

    base = step_id * SEQ_BLOCK
    slots = lat_in.shape[2]
    row_l = lax.broadcasted_iota(jnp.int32, (slots, lora), 0)
    row_r = lax.broadcasted_iota(jnp.int32, (slots, rope), 0)
    step = (lax.broadcasted_iota(jnp.int32, (queries, slots), 0) >= heads).astype(jnp.int32)
    slot = lax.broadcasted_iota(jnp.int32, (queries, slots), 1)
    for first in range(0, SEQ_BLOCK, SEQ_GROUP):
        group = range(first, first + SEQ_GROUP)
        lats, scores = {}, {}
        for i in group:
            p = pos_smem[base + i]
            lat = lat_in[0, i].astype(jnp.float32)
            rop = rope_in[0, i].astype(jnp.float32)
            for s in range(2):
                lat = jnp.where(row_l == p + s, ln_s[pl.ds(s * seqs + base + i, 1), :], lat)
                rop = jnp.where(row_r == p + s, rn_s[pl.ds(s * seqs + base + i, 1), :], rop)
            lats[i] = lat.astype(jnp.bfloat16)
            rop = rop.astype(jnp.bfloat16)
            lat_out[0, i] = lats[i]
            rope_out[0, i] = rop
            sc = fdot_t(q_s[base + i].astype(jnp.bfloat16), lats[i]) + fdot_t(qp_s[base + i].astype(jnp.bfloat16), rop)
            scores[i] = jnp.where(slot <= p + step, sc * scale, -1e30)
        peaks = {i: jnp.max(scores[i], axis=-1, keepdims=True) for i in group}
        exps = {i: jnp.exp(scores[i] - peaks[i]) for i in group}
        sums = {i: jnp.sum(exps[i], axis=-1, keepdims=True) for i in group}
        for i in group:
            o_s[base + i] = fdot((exps[i] / sums[i]).astype(jnp.bfloat16), lats[i])

    @pl.when(step_id == pl.num_programs(0) - 1)
    def _():
        outs = []
        for n in range(heads):
            o = jnp.concatenate([o_s[:, n, :], o_s[:, heads + n, :]], axis=0).astype(jnp.bfloat16)
            outs.append(fdot(o, w_uv[0, :, n, :]).astype(jnp.bfloat16))
        o = jnp.concatenate(outs, axis=1)
        for c in range(0, w_o.shape[2], 512):
            part[:, c:c + 512] = fdot(o, w_o[0, :, c:c + 512])


def attn_block(layer, pos, h, gain, kv_gain, cos, sin, w_q, w_kv, w_uk, w_uv, w_o, lat_cache, rope_cache, prev):
    _, seqs, slots, lora = lat_cache.shape
    rope = rope_cache.shape[3]
    rows, hidden = h.shape
    heads, qk = w_q.shape[1], w_q.shape[2]
    vm = pl.BlockSpec(memory_space=VMEM)
    lay = lambda *tail: pl.BlockSpec((1, SEQ_BLOCK) + tail, lambda i: (layer, i, 0, 0))
    wt = lambda w: pl.BlockSpec((1,) + w.shape[1:], lambda i: (layer,) + (0,) * (w.ndim - 1), pipeline_mode=pl.Buffered(1))
    weights = [w_q, w_kv, w_uk, w_uv, w_o]
    in_specs = [pl.BlockSpec(memory_space=pltpu.SMEM)] + [vm] * 5 + [wt(w) for w in weights] + [lay(slots, lora), lay(slots, rope)]
    args = [pos, h, gain, kv_gain, cos, sin] + weights + [lat_cache, rope_cache]
    alias = {}
    if prev is not None:
        alias = {len(args): 0, len(args) + 1: 1}
        in_specs += [pl.BlockSpec(memory_space=pl.ANY)] * 2
        args += list(prev)
    f32 = lambda *s: VMEM(s, jnp.float32)
    lat, rop, part = pl.pallas_call(
        functools.partial(attn_kernel, layer, 1.0 / math.sqrt(qk)),
        grid=(seqs // SEQ_BLOCK,),
        out_shape=(jax.ShapeDtypeStruct(lat_cache.shape, jnp.bfloat16), jax.ShapeDtypeStruct(rope_cache.shape, jnp.bfloat16), jax.ShapeDtypeStruct((rows, hidden), jnp.float32)),
        in_specs=in_specs,
        out_specs=(lay(slots, lora), lay(slots, rope), vm),
        scratch_shapes=[VMEM((rows, hidden), jnp.bfloat16), f32(seqs, 2 * heads, lora), f32(seqs, 2 * heads, rope), f32(rows, lora), f32(rows, rope), f32(seqs, 2 * heads, lora)],
        input_output_aliases=alias,
        compiler_params=pltpu.CompilerParams(dimension_semantics=("arbitrary",), vmem_limit_bytes=VMEM_CAP),
        name=f"attn{layer}",
    )(*args)
    return part, (lat, rop)


def barrier(z, ends, extra):
    sem = pltpu.get_barrier_semaphore()

    @pl.when(z > 0)
    def _():
        pl.semaphore_signal(sem, inc=1, device_id={"tp": z - 1}, device_id_type=MESH)

    @pl.when(z < ends)
    def _():
        pl.semaphore_signal(sem, inc=1, device_id={"tp": z + 1}, device_id_type=MESH)

    for dev in extra:
        pl.semaphore_signal(sem, inc=1, device_id=dev, device_id_type=MESH)
    count = len(extra) + jnp.where(z > 0, 1, 0) + jnp.where(z < ends, 1, 0)
    pl.semaphore_wait(sem, count)


class Line:
    def __init__(self, z, ends, chunks, src, buf, out, residual, sems):
        self.z, self.ends, self.chunks = z, ends, chunks
        self.src, self.buf, self.out, self.residual = src, buf, out, residual
        self.rs_s, self.rs_r, self.bc_s, self.bc_r = sems
        self.rows = src.shape[0] // (2 * chunks)
        low = 2 * z < ends
        self.near = jnp.where(low, 1, 0)
        self.far = 1 - self.near
        self.near_at = jnp.where(low, z, ends - z)
        self.far_at = ends - self.near_at
        up, down = jnp.minimum(z + 1, ends), jnp.maximum(z - 1, 0)
        self.inward = jnp.where(low, up, down)
        self.outward = jnp.where(low, down, up)

    def ready(self, d, c):
        pass

    def sl(self, d, c):
        return pl.ds(pl.multiple_of((d * self.chunks + c) * self.rows, self.rows), self.rows)

    def rs(self, d, c, src, dev):
        return pltpu.make_async_remote_copy(src_ref=src, dst_ref=self.buf.at[d, c], send_sem=self.rs_s.at[d, c], recv_sem=self.rs_r.at[d, c], device_id={"tp": dev}, device_id_type=MESH)

    def bc(self, d, c, dev):
        ref = self.out.at[self.sl(d, c)]
        return pltpu.make_async_remote_copy(src_ref=ref, dst_ref=ref, send_sem=self.bc_s.at[d, c], recv_sem=self.bc_r.at[d, c], device_id={"tp": dev}, device_id_type=MESH)

    def reduce_near(self, c):
        d, sl, src, buf = self.near, self.sl(self.near, c), self.src, self.buf

        @pl.when(self.near_at == 0)
        def _():
            self.rs(d, c, src.at[sl], self.inward).start()

        @pl.when(self.near_at > 0)
        def _():
            self.rs(d, c, src.at[sl], self.inward).wait_recv()
            buf[d, c] = buf[d, c] + src[sl]
            self.rs(d, c, buf.at[d, c], self.inward).start()

    def reduce_far(self, c):
        d, sl, src, buf = self.far, self.sl(self.far, c), self.src, self.buf

        @pl.when(self.near_at > 0)
        def _():
            self.rs(d, c, src.at[sl], self.outward).wait_recv()
            buf[d, c] = buf[d, c] + src[sl]
            self.rs(d, c, buf.at[d, c], self.outward).start()

    def finish_far(self, c):
        d, sl, src, buf = self.far, self.sl(self.far, c), self.src, self.buf

        @pl.when(self.near_at == 0)
        def _():
            self.rs(d, c, src.at[sl], self.outward).wait_recv()
            self.out[sl] = (self.residual[sl].astype(jnp.float32) + (buf[d, c] + src[sl])).astype(jnp.bfloat16)
            self.bc(d, c, self.inward).start()
            self.ready(d, c)

    def spread_far(self, c):
        @pl.when(self.near_at > 0)
        def _():
            self.bc(self.far, c, self.inward).wait_recv()
            self.bc(self.far, c, self.inward).start()
            self.ready(self.far, c)

    def spread_near(self, c):
        @pl.when(self.near_at > 0)
        def _():
            self.bc(self.near, c, self.outward).wait_recv()
            self.bc(self.near, c, self.outward).start()
            self.ready(self.near, c)

    def finish_near(self, c):
        @pl.when(self.near_at == 0)
        def _():
            self.bc(self.near, c, self.outward).wait_recv()
            self.ready(self.near, c)

    def drain(self, c):
        self.rs(self.near, c, self.src.at[self.sl(self.near, c)], self.inward).wait_send()
        self.bc(self.far, c, self.inward).wait_send()

        @pl.when(self.near_at > 0)
        def _():
            self.rs(self.far, c, self.src.at[self.sl(self.far, c)], self.outward).wait_send()
            self.bc(self.near, c, self.outward).wait_send()

    def stage(self, t, lags=LAGS):
        for fn, lag in ((self.reduce_near, 0), (self.reduce_far, lags[0]), (self.finish_far, lags[1]), (self.spread_far, lags[2]), (self.spread_near, lags[3]), (self.finish_near, lags[4])):
            if 0 <= t - lag < self.chunks:
                fn(t - lag)

    def run(self):
        for t in range(self.chunks + max(LAGS)):
            self.stage(t)
        for c in range(self.chunks):
            self.drain(c)


def line_scratch(rows, tail, chunks=CHUNKS):
    return [VMEM((2, chunks, rows // (2 * chunks)) + tail, jnp.float32)] + [DMA((2, chunks)) for _ in range(4)]


def norm_rows(src, gain, dst, step=32):
    for r in range(0, src.shape[0], step):
        dst[r:r + step, :] = rms_norm(src[r:r + step, :], gain[...])


def fdot_t(a, b):
    return lax.dot_general(a, b, (((1,), (1,)), ((), ())), preferred_element_type=jnp.float32)


def mlp_act(x, gate, up, act, block):
    def body(j, carry):
        js = pl.ds(pl.multiple_of(j * block, 16), block)
        g = fdot_t(gate[js, :], x[...])
        u = fdot_t(up[js, :], x[...])
        act[js, :] = (g * jax.nn.sigmoid(g) * u).astype(jnp.bfloat16)
        return carry

    lax.fori_loop(0, gate.shape[0] // block, body, 0)


def mlp_down(act, act_t, down, put):
    act_t[...] = act[...].T

    def body(j, carry):
        ns = pl.ds(pl.multiple_of(j * 512, 512), 512)
        put(ns, fdot(act_t[...], down[:, ns]))
        return carry

    lax.fori_loop(0, down.shape[1] // 512, body, 0)


def load(pairs, sem):
    copies = []
    for k, (src, dst) in enumerate(pairs):
        cp = pltpu.make_async_copy(src, dst, sem.at[k])
        cp.start()
        copies.append(cp)
    return copies


def dense_kernel(part, res, gain, ids, w_gate, w_up, w_down, h_out, ids_out, y, x, gate, up, down, act, act_t, part2, id_s, id_r, w_sem, *line):
    z, e = lax.axis_index("tp"), lax.axis_index("ep")
    ends = lax.axis_size("tp") - 1
    width = gate.shape[0]
    loads = load([(w_gate, gate), (w_up, up), (w_down, down)], w_sem)
    n_ep = lax.axis_size("ep")
    peers = [{"ep": lax.rem(e + k, n_ep)} for k in range(1, n_ep)]
    barrier(z, ends, peers)
    sends = []
    for k, dev in enumerate(peers):
        cp = pltpu.make_async_remote_copy(src_ref=ids, dst_ref=ids_out.at[e], send_sem=id_s.at[k], recv_sem=id_r.at[k], device_id=dev, device_id_type=MESH)
        cp.start()
        sends.append(cp)
    ids_out[e] = ids[...]
    one = Line(z, ends, CHUNKS, part, line[0], y, res, line[1:5])

    def normed(d, c):
        x[one.sl(d, c)] = rms_norm(y[one.sl(d, c)], gain[0:1, :])

    one.ready = normed
    one.run()
    loads[0].wait()
    loads[1].wait()
    mlp_act(x, gate, up, act, width // 3)
    loads[2].wait()

    def put(ns, v):
        part2[:, ns] = v

    mlp_down(act, act_t, down, put)
    two = Line(z, ends, CHUNKS, part2, line[5], h_out, y, line[6:10])
    two.run()
    for cp in sends:
        cp.wait()


def dense_block(part, res, gain, ids, w_gate, w_up, w_down):
    rows, hidden = part.shape
    width = w_gate.shape[0]
    vm = pl.BlockSpec(memory_space=VMEM)
    hbm = pl.BlockSpec(memory_space=pl.ANY)
    bf = lambda *s: jax.ShapeDtypeStruct(s, jnp.bfloat16)
    line = line_scratch(rows, (hidden,))
    return pl.pallas_call(
        dense_kernel,
        out_shape=(bf(rows, hidden), jax.ShapeDtypeStruct((4,) + ids.shape, jnp.int32)),
        in_specs=[vm] * 4 + [hbm] * 3,
        out_specs=(vm, vm),
        scratch_shapes=[VMEM((rows, hidden), jnp.bfloat16), VMEM((rows, hidden), jnp.bfloat16), VMEM((width, hidden), jnp.bfloat16), VMEM((width, hidden), jnp.bfloat16), VMEM((width, hidden), jnp.bfloat16), VMEM((width, rows), jnp.bfloat16), VMEM((rows, width), jnp.bfloat16), VMEM((rows, hidden), jnp.float32), DMA((3,)), DMA((3,)), DMA((3,))] + line + line,
        compiler_params=pltpu.CompilerParams(collective_id=1, has_side_effects=True, vmem_limit_bytes=VMEM_CAP),
        name="dense",
    )(part, res, gain, ids, w_gate, w_up, w_down)


def gather_kernel(part, res, gain, router, w_gate, w_up, w_down, y, x_all, shared, probs, gate, up, down, act, act_t, w_sem, c_s, c_r, y_s, y_r, f_s, f_r, *line):
    z, e = lax.axis_index("tp"), lax.axis_index("ep")
    ends = lax.axis_size("tp") - 1
    width = gate.shape[0]
    rows, hidden = y.shape
    loads = load([(w_gate, gate), (w_up, up), (w_down, down)], w_sem)
    core, chip = jnp.bitwise_xor(e, 1), jnp.bitwise_xor(e, 2)
    barrier(z, ends, [{"ep": core}, {"ep": chip}])
    one = Line(z, ends, CHUNKS, part, line[0], y, res, line[1:5])
    mine = x_all.at[e]

    def copy(src, dst, ss, rs, dev):
        return pltpu.make_async_remote_copy(src_ref=src, dst_ref=dst, send_sem=ss, recv_sem=rs, device_id={"ep": dev}, device_id_type=MESH)

    def to_chip(d, c):
        ref = x_all.at[e, one.sl(d, c)]
        return copy(ref, ref, y_s.at[d, c], y_r.at[d, c], chip)

    def to_core(d, c):
        ref = x_all.at[chip, one.sl(d, c)]
        return copy(ref, ref, f_s.at[d, c], f_r.at[d, c], core)

    def normed(d, c):
        x_all[e, one.sl(d, c)] = rms_norm(y[one.sl(d, c)], gain[1:2, :])
        to_chip(d, c).start()

    one.ready = normed
    one.run()
    own = copy(mine, mine, c_s, c_r, core)
    own.start()
    loads[0].wait()
    loads[1].wait()
    mlp_act(mine, gate, up, act, width // 2)
    loads[2].wait()

    def put(ns, v):
        for j in range(4):
            shared[:, ns.start // 128 + j, :] = v[:, j * 128:(j + 1) * 128]

    mlp_down(act, act_t, down, put)
    def route(j):
        logits = fdot_t(router[...], x_all[j])
        e_x = jnp.exp(logits - jnp.max(logits, axis=0, keepdims=True))
        probs[:, pl.ds(pl.multiple_of(j * rows, rows), rows)] = e_x / jnp.sum(e_x, axis=0, keepdims=True)

    route(e)
    every = [(d, c) for c in range(CHUNKS) for d in range(2)]
    for d, c in every:
        to_chip(d, c).wait_recv()
        to_core(d, c).start()
    route(chip)
    own.wait()
    route(core)
    for d, c in every:
        to_chip(d, c).wait_send()
        to_core(d, c).wait()
    route(jnp.bitwise_xor(e, 3))


def gather_block(part, res, gain, router, w_gate, w_up, w_down):
    rows, hidden = part.shape
    width = w_gate.shape[0]
    vm = pl.BlockSpec(memory_space=VMEM)
    hbm = pl.BlockSpec(memory_space=pl.ANY)
    return pl.pallas_call(
        gather_kernel,
        out_shape=(jax.ShapeDtypeStruct((rows, hidden), jnp.bfloat16), jax.ShapeDtypeStruct((4, rows, hidden), jnp.bfloat16), jax.ShapeDtypeStruct((rows, hidden // 128, 128), jnp.float32), jax.ShapeDtypeStruct((router.shape[0], 4 * rows), jnp.float32)),
        in_specs=[vm] * 4 + [hbm] * 3,
        out_specs=(vm, vm, vm, vm),
        scratch_shapes=[VMEM((width, hidden), jnp.bfloat16), VMEM((width, hidden), jnp.bfloat16), VMEM((width, hidden), jnp.bfloat16), VMEM((width, rows), jnp.bfloat16), VMEM((rows, width), jnp.bfloat16), DMA((3,)), DMA, DMA] + [DMA((2, CHUNKS)) for _ in range(4)] + line_scratch(rows, (hidden,)),
        compiler_params=pltpu.CompilerParams(collective_id=2, has_side_effects=True, vmem_limit_bytes=VMEM_CAP),
        name="gather",
    )(part, res, gain, router, w_gate, w_up, w_down)


def expert_kernel(own, counts, lists, weights, x_all, shared, w_gate, w_up, w_down, acc, acc_s, x3, rows3, xb, d2, d3):
    e = pl.program_id(0)
    tokens, slabs = x3.shape[0], x3.shape[1]
    local = pl.num_programs(0)

    @pl.when(e == 0)
    def _():
        acc_s[...] = jnp.zeros_like(acc_s)
        xb[...] = jnp.zeros_like(xb)
        acc_s[pl.ds(own[0] * shared.shape[0], shared.shape[0])] = shared[...]

        def widen(i, carry):
            r = pl.ds(pl.multiple_of(i * 64, 64), 64)
            for k in range(slabs):
                x3[r, k, :] = x_all[r, k * 128:(k + 1) * 128].astype(jnp.float32)
            return carry

        lax.fori_loop(0, tokens // 64, widen, 0)

    n = counts[e]

    def tile(i, carry):
        first = i * ROW_TILE
        left = jnp.minimum(n - i * ROW_TILE, ROW_TILE)
        groups = (left + GROUP - 1) // GROUP

        def fetch(g, c):
            sl = pl.ds(pl.multiple_of(g * GROUP, GROUP), GROUP)
            for r in range(GROUP):
                rows3[g * GROUP + r] = x3[lists[e, first + g * GROUP + r]]
            for k in range(slabs):
                xb[sl, k * 128:(k + 1) * 128] = rows3[sl, k, :].astype(jnp.bfloat16)
            return c

        lax.fori_loop(0, groups, fetch, 0)
        g = fdot_t(w_gate[0], xb[...])
        u = fdot_t(w_up[0], xb[...])
        act = (g * jax.nn.sigmoid(g) * u).T.astype(jnp.bfloat16)
        for c in range(0, slabs, 4):
            d2[:, c * 128:(c + 4) * 128] = fdot(act, w_down[0, :, c * 128:(c + 4) * 128])

        def scatter(g, c):
            sl = pl.ds(pl.multiple_of(g * GROUP, GROUP), GROUP)
            for k in range(slabs):
                d3[:, k, :] = d2[sl, k * 128:(k + 1) * 128]
            ts = []
            for r in range(GROUP):
                ok = g * GROUP + r < left
                ts.append(jnp.where(ok, lists[e, first + g * GROUP + r], tokens))
            vals = [acc_s[ts[r]] + weights[e, jnp.minimum(ts[r], tokens - 1)] * d3[r] for r in range(GROUP)]
            for r in range(GROUP):
                acc_s[ts[r]] = vals[r]
            return c

        lax.fori_loop(0, groups, scatter, 0)
        return carry

    lax.fori_loop(0, (n + ROW_TILE - 1) // ROW_TILE, tile, 0)

    @pl.when(e == local - 1)
    def _():
        acc[...] = acc_s[pl.ds(0, tokens)]


def expert_block(own, counts, lists, weights, x_all, shared, w_gate, w_up, w_down):
    tokens, hidden = x_all.shape
    local, width, _ = w_gate.shape
    slabs = hidden // 128
    sm = pl.BlockSpec(memory_space=pltpu.SMEM)
    vm = pl.BlockSpec(memory_space=VMEM)
    return pl.pallas_call(
        expert_kernel,
        grid=(local,),
        out_shape=jax.ShapeDtypeStruct((tokens, slabs, 128), jnp.float32),
        in_specs=[sm, sm, sm, sm, vm, vm, pl.BlockSpec((1, width, hidden), lambda e: (e, 0, 0)), pl.BlockSpec((1, width, hidden), lambda e: (e, 0, 0)), pl.BlockSpec((1, width, hidden), lambda e: (e, 0, 0))],
        out_specs=vm,
        scratch_shapes=[VMEM((tokens + 8, slabs, 128), jnp.float32), VMEM((tokens, slabs, 128), jnp.float32), VMEM((ROW_TILE, slabs, 128), jnp.float32), VMEM((ROW_TILE, hidden), jnp.bfloat16), VMEM((ROW_TILE, hidden), jnp.float32), VMEM((GROUP, slabs, 128), jnp.float32)],
        compiler_params=pltpu.CompilerParams(dimension_semantics=("arbitrary",), vmem_limit_bytes=VMEM_CAP),
        name="experts",
    )(own, counts, lists, weights, x_all, shared, w_gate, w_up, w_down)


def combine_kernel(acc, res, out, total, from_core, from_chip, own_sum, c_s, c_r, y_s, y_r, *line):
    z, e = lax.axis_index("tp"), lax.axis_index("ep")
    ends = lax.axis_size("tp") - 1
    core, chip = jnp.bitwise_xor(e, 1), jnp.bitwise_xor(e, 2)
    both = jnp.bitwise_xor(e, 3)
    barrier(z, ends, [{"ep": core}, {"ep": chip}])
    rows = res.shape[0]
    step = rows // (2 * COMBINE_CHUNKS)
    order = [(d, c) for c in range(COMBINE_CHUNKS) for d in range(2)]

    def copy(src, dst, ss, rs, dev):
        return pltpu.make_async_remote_copy(src_ref=src, dst_ref=dst, send_sem=ss, recv_sem=rs, device_id={"ep": dev}, device_id_type=MESH)

    hops = []
    for w, block in enumerate((both, core)):
        for d, c in order:
            k = d * COMBINE_CHUNKS + c
            cp = copy(acc.at[pl.ds(block * rows + k * step, step)], from_core.at[w, pl.ds(k * step, step)], c_s.at[w, k], c_r.at[w, k], core)
            cp.start()
            hops.append(cp)
    n = len(order)
    outs = []
    for j, (d, c) in enumerate(order):
        k = d * COMBINE_CHUNKS + c
        hops[j].wait_recv()
        sl = pl.ds(k * step, step)
        total[sl] = acc[pl.ds(chip * rows + k * step, step)] + from_core[0, sl]
        cp = copy(total.at[sl], from_chip.at[sl], y_s.at[k], y_r.at[k], chip)
        cp.start()
        outs.append(cp)
    one = Line(z, ends, COMBINE_CHUNKS, own_sum, line[0], out, res, line[1:5])
    for t in range(COMBINE_CHUNKS + max(COMBINE_LAGS)):
        for j in (2 * t, 2 * t + 1):
            if j < n:
                d, c = order[j]
                sl = pl.ds((d * COMBINE_CHUNKS + c) * step, step)
                hops[n + j].wait_recv()
                outs[j].wait_recv()
                own_sum[sl] = (acc[pl.ds(e * rows + (d * COMBINE_CHUNKS + c) * step, step)] + from_core[1, sl]) + from_chip[sl]
        one.stage(t, COMBINE_LAGS)
    for c in range(COMBINE_CHUNKS):
        one.drain(c)
    for cp in hops + outs:
        cp.wait_send()


def combine_block(acc, res):
    rows, slabs, lanes = res.shape
    vm = pl.BlockSpec(memory_space=VMEM)
    f32 = lambda *s: VMEM(s, jnp.float32)
    n = 2 * COMBINE_CHUNKS
    return pl.pallas_call(
        combine_kernel,
        out_shape=jax.ShapeDtypeStruct(res.shape, jnp.bfloat16),
        in_specs=[vm, vm],
        out_specs=vm,
        scratch_shapes=[f32(rows, slabs, lanes), f32(2, rows, slabs, lanes), f32(rows, slabs, lanes), f32(rows, slabs, lanes), DMA((2, n)), DMA((2, n)), DMA((n,)), DMA((n,))] + line_scratch(rows, (slabs, lanes), COMBINE_CHUNKS),
        compiler_params=pltpu.CompilerParams(collective_id=3, has_side_effects=True, vmem_limit_bytes=VMEM_CAP),
        name="combine",
    )(acc, res)


def token_lists(ids, ep, local):
    tokens = ids.shape[0]
    mine = jnp.any(ids[:, :, None] == (ep * local + jnp.arange(local))[None, None, :], axis=1)
    lower = (jnp.arange(tokens)[:, None] > jnp.arange(tokens)[None, :]).astype(jnp.bfloat16)
    rank = fdot(lower, mine.astype(jnp.bfloat16)).astype(jnp.int32)
    rank = jnp.where(mine, rank, -1)
    hit = rank.T[:, None, :] == jnp.arange(tokens)[None, :, None]
    lists = jnp.sum(jnp.where(hit, jnp.arange(tokens)[None, None, :], 0), axis=2)
    counts = jnp.sum(mine.astype(jnp.int32), axis=0)
    return lists.astype(jnp.int32), counts


def solution(mesh):
    tok_axes = ('dp', 'ep')

    def device_fn(emb, pos, route_ids, lat_cache, rope_cache, attn_norm, w_q, w_dkv, kv_norm, w_uk, w_uv, w_o, mlp_norm, dense_gate, dense_up, dense_down, router, shared_gate, shared_up, shared_down, expert_gate, expert_up, expert_down):
        _, seqs, hidden = emb.shape
        rows = 2 * seqs
        ep = lax.axis_index('ep')
        n_ep = lax.axis_size('ep')
        local = expert_gate.shape[0]
        top_k = route_ids.shape[2]
        cur = jnp.concatenate([pos, pos + 1])
        cos_t, sin_t = rope_tables(cur, rope_cache.shape[-1])
        h0 = emb.reshape(rows, hidden)
        weights = (w_q.transpose(0, 2, 3, 1), w_dkv.swapaxes(1, 2), w_uk, w_uv, w_o, lat_cache, rope_cache)
        attn = lambda layer, h, prev: attn_block(layer, pos, h, attn_norm, kv_norm, cos_t.T, sin_t.T, *weights, prev)
        part, caches = attn(0, h0, None)
        flat = route_ids.reshape(-1)
        ids = jnp.pad(flat, (0, -flat.size % 1024)).reshape(-1, 128)
        h_mid, ids_all = dense_block(part, h0, mlp_norm, ids, dense_gate.T, dense_up.T, dense_down)
        ids_all = ids_all.reshape(n_ep, -1)[:, :flat.size].reshape(n_ep * rows, top_k)
        lists, counts = token_lists(ids_all, ep, local)
        part, caches = attn(1, h_mid, caches)
        y, x_all, shared, probs = gather_block(part, h_mid, mlp_norm, router.T, shared_gate.T, shared_up.T, shared_down)
        x_all = x_all.reshape(n_ep * rows, hidden)
        weights = lax.dynamic_slice_in_dim(probs, ep * local, local, axis=0)
        acc = expert_block(ep.reshape(1), counts, lists, weights, x_all, shared, expert_gate.swapaxes(1, 2), expert_up.swapaxes(1, 2), expert_down)
        out = combine_block(acc, y.reshape(rows, hidden // 128, 128))
        return out.reshape(2, seqs, hidden), caches[0], caches[1]

    in_specs = (P(None, tok_axes, None), P(tok_axes), P(None, tok_axes, None), P(None, tok_axes, None, None), P(None, tok_axes, None, None), P(), P(None, None, 'tp', None), P(), P(), P(None, None, 'tp', None), P(None, None, 'tp', None), P(None, 'tp', None), P(), P(None, 'tp'), P(None, 'tp'), P('tp', None), P(), P(None, 'tp'), P(None, 'tp'), P('tp', None), P('ep', None, 'tp'), P('ep', None, 'tp'), P('ep', 'tp', None))
    out_specs = (P(None, tok_axes, None), P(None, tok_axes, None, None), P(None, tok_axes, None, None))
    return jax.shard_map(device_fn, mesh=mesh, in_specs=in_specs, out_specs=out_specs, check_vma=False)
```

```python
import functools
import math
import jax
import jax.numpy as jnp
from jax import lax
from jax.experimental import pallas as pl
from jax.experimental.pallas import tpu as pltpu
from jax.sharding import PartitionSpec as P

NORM_EPS = 1e-6
ROPE_THETA = 10000.0
MESH = pl.DeviceIdType.MESH
VMEM = pltpu.VMEM
DMA = pltpu.SemaphoreType.DMA
VMEM_CAP = 62 * 1024 * 1024
SEQ_BLOCK = 16
SEQ_GROUP = 8
CHUNKS = 8
LAGS = (2, 8, 7, 9, 18, 0)
COMBINE_CHUNKS = 8
COMBINE_LAGS = (3, 5, 6, 8, 16, 1)
ROW_TILE = 128
GROUP = 16


def rms_norm(values, gain):
    wide = values.astype(jnp.float32)
    mean_sq = jnp.mean(wide * wide, axis=-1, keepdims=True)
    return (wide * lax.rsqrt(mean_sq + NORM_EPS) * gain).astype(jnp.bfloat16)


def rope_tables(position, rope_dim):
    half_dim = rope_dim // 2
    inv_freq = ROPE_THETA ** (-(jnp.arange(half_dim, dtype=jnp.float32) * 2.0 / rope_dim))
    angles = position.astype(jnp.float32)[:, None] * inv_freq[None, :]
    return jnp.cos(angles), jnp.sin(angles)


def fdot(a, b):
    return jnp.dot(a, b, preferred_element_type=jnp.float32)


def rotate_t(v, cos, sin):
    half = v.shape[0] // 2
    first, second = v[:half], v[half:]
    return jnp.concatenate([first * cos - second * sin, second * cos + first * sin], axis=0)


def rounded(v):
    return v.astype(jnp.bfloat16).astype(jnp.float32)


def attn_kernel(layer, scale, pos_smem, h, gain, kv_gain, cos, sin, w_q, w_kv, w_uk, w_uv, w_o, lat_in, rope_in, *rest):
    lat_out, rope_out, part, x, q_s, qp_s, ln_s, rn_s, o_s = rest[-9:]
    step_id = pl.program_id(0)
    heads, qk = w_q.shape[1], w_q.shape[2]
    seqs, queries, lora = q_s.shape
    rope = rope_in.shape[3]
    nope = qk - rope

    @pl.when(step_id == 0)
    def _():
        norm_rows(h, gain.at[layer:layer + 1], x)
        kv = fdot_t(w_kv[0], x[...])
        lat = kv[:lora]
        lat = lat * lax.rsqrt(jnp.mean(lat * lat, axis=0, keepdims=True) + NORM_EPS)
        ln_s[...] = rounded(lat.T * kv_gain[layer:layer + 1, :])
        rn_s[...] = rounded(rotate_t(kv[lora:], cos[...], sin[...])).T
        for n in range(heads):
            q = fdot_t(w_q[0, n], x[...])
            q_nope = q[:nope].T.astype(jnp.bfloat16)
            q_pe = rotate_t(q[nope:], cos[...], sin[...]).T
            q_lat = fdot_t(q_nope, w_uk[0, :, n, :])
            for s in range(2):
                q_s[:, s * heads + n, :] = q_lat[s * seqs:(s + 1) * seqs]
                qp_s[:, s * heads + n, :] = q_pe[s * seqs:(s + 1) * seqs]

    base = step_id * SEQ_BLOCK
    slots = lat_in.shape[2]
    row_l = lax.broadcasted_iota(jnp.int32, (slots, lora), 0)
    row_r = lax.broadcasted_iota(jnp.int32, (slots, rope), 0)
    step = (lax.broadcasted_iota(jnp.int32, (queries, slots), 0) >= heads).astype(jnp.int32)
    slot = lax.broadcasted_iota(jnp.int32, (queries, slots), 1)
    for first in range(0, SEQ_BLOCK, SEQ_GROUP):
        group = range(first, first + SEQ_GROUP)
        lats, scores = {}, {}
        for i in group:
            p = pos_smem[base + i]
            lat = lat_in[0, i].astype(jnp.float32)
            rop = rope_in[0, i].astype(jnp.float32)
            for s in range(2):
                lat = jnp.where(row_l == p + s, ln_s[pl.ds(s * seqs + base + i, 1), :], lat)
                rop = jnp.where(row_r == p + s, rn_s[pl.ds(s * seqs + base + i, 1), :], rop)
            lats[i] = lat.astype(jnp.bfloat16)
            rop = rop.astype(jnp.bfloat16)
            lat_out[0, i] = lats[i]
            rope_out[0, i] = rop
            sc = fdot_t(q_s[base + i].astype(jnp.bfloat16), lats[i]) + fdot_t(qp_s[base + i].astype(jnp.bfloat16), rop)
            scores[i] = jnp.where(slot <= p + step, sc * scale, -1e30)
        peaks = {i: jnp.max(scores[i], axis=-1, keepdims=True) for i in group}
        exps = {i: jnp.exp(scores[i] - peaks[i]) for i in group}
        sums = {i: jnp.sum(exps[i], axis=-1, keepdims=True) for i in group}
        for i in group:
            o_s[base + i] = fdot((exps[i] / sums[i]).astype(jnp.bfloat16), lats[i])

    @pl.when(step_id == pl.num_programs(0) - 1)
    def _():
        outs = []
        for n in range(heads):
            o = jnp.concatenate([o_s[:, n, :], o_s[:, heads + n, :]], axis=0).astype(jnp.bfloat16)
            outs.append(fdot(o, w_uv[0, :, n, :]).astype(jnp.bfloat16))
        o = jnp.concatenate(outs, axis=1)
        for c in range(0, w_o.shape[2], 512):
            part[:, c:c + 512] = fdot(o, w_o[0, :, c:c + 512])


def attn_block(layer, pos, h, gain, kv_gain, cos, sin, w_q, w_kv, w_uk, w_uv, w_o, lat_cache, rope_cache, prev):
    _, seqs, slots, lora = lat_cache.shape
    rope = rope_cache.shape[3]
    rows, hidden = h.shape
    heads, qk = w_q.shape[1], w_q.shape[2]
    vm = pl.BlockSpec(memory_space=VMEM)
    lay = lambda *tail: pl.BlockSpec((1, SEQ_BLOCK) + tail, lambda i: (layer, i, 0, 0))
    wt = lambda w: pl.BlockSpec((1,) + w.shape[1:], lambda i: (layer,) + (0,) * (w.ndim - 1), pipeline_mode=pl.Buffered(1))
    weights = [w_q, w_kv, w_uk, w_uv, w_o]
    in_specs = [pl.BlockSpec(memory_space=pltpu.SMEM)] + [vm] * 5 + [wt(w) for w in weights] + [lay(slots, lora), lay(slots, rope)]
    args = [pos, h, gain, kv_gain, cos, sin] + weights + [lat_cache, rope_cache]
    alias = {}
    if prev is not None:
        alias = {len(args): 0, len(args) + 1: 1}
        in_specs += [pl.BlockSpec(memory_space=pl.ANY)] * 2
        args += list(prev)
    f32 = lambda *s: VMEM(s, jnp.float32)
    lat, rop, part = pl.pallas_call(
        functools.partial(attn_kernel, layer, 1.0 / math.sqrt(qk)),
        grid=(seqs // SEQ_BLOCK,),
        out_shape=(jax.ShapeDtypeStruct(lat_cache.shape, jnp.bfloat16), jax.ShapeDtypeStruct(rope_cache.shape, jnp.bfloat16), jax.ShapeDtypeStruct((rows, hidden), jnp.float32)),
        in_specs=in_specs,
        out_specs=(lay(slots, lora), lay(slots, rope), vm),
        scratch_shapes=[VMEM((rows, hidden), jnp.bfloat16), f32(seqs, 2 * heads, lora), f32(seqs, 2 * heads, rope), f32(rows, lora), f32(rows, rope), f32(seqs, 2 * heads, lora)],
        input_output_aliases=alias,
        compiler_params=pltpu.CompilerParams(dimension_semantics=("arbitrary",), vmem_limit_bytes=VMEM_CAP),
        name=f"attn{layer}",
    )(*args)
    return part, (lat, rop)


def barrier(z, ends, extra):
    sem = pltpu.get_barrier_semaphore()

    @pl.when(z > 0)
    def _():
        pl.semaphore_signal(sem, inc=1, device_id={"tp": z - 1}, device_id_type=MESH)

    @pl.when(z < ends)
    def _():
        pl.semaphore_signal(sem, inc=1, device_id={"tp": z + 1}, device_id_type=MESH)

    for dev in extra:
        pl.semaphore_signal(sem, inc=1, device_id=dev, device_id_type=MESH)
    count = len(extra) + jnp.where(z > 0, 1, 0) + jnp.where(z < ends, 1, 0)
    pl.semaphore_wait(sem, count)


class Line:
    def __init__(self, z, ends, chunks, src, buf, out, residual, sems):
        self.z, self.ends, self.chunks = z, ends, chunks
        self.src, self.buf, self.out, self.residual = src, buf, out, residual
        self.rs_s, self.rs_r, self.bc_s, self.bc_r = sems
        self.rows = src.shape[0] // (2 * chunks)
        low = 2 * z < ends
        self.near = jnp.where(low, 1, 0)
        self.far = 1 - self.near
        self.near_at = jnp.where(low, z, ends - z)
        self.far_at = ends - self.near_at
        up, down = jnp.minimum(z + 1, ends), jnp.maximum(z - 1, 0)
        self.inward = jnp.where(low, up, down)
        self.outward = jnp.where(low, down, up)

    def ready(self, d, c):
        pass

    def sl(self, d, c):
        return pl.ds(pl.multiple_of((d * self.chunks + c) * self.rows, self.rows), self.rows)

    def rs(self, d, c, src, dev):
        return pltpu.make_async_remote_copy(src_ref=src, dst_ref=self.buf.at[d, c], send_sem=self.rs_s.at[d, c], recv_sem=self.rs_r.at[d, c], device_id={"tp": dev}, device_id_type=MESH)

    def bc(self, d, c, dev):
        ref = self.out.at[self.sl(d, c)]
        return pltpu.make_async_remote_copy(src_ref=ref, dst_ref=ref, send_sem=self.bc_s.at[d, c], recv_sem=self.bc_r.at[d, c], device_id={"tp": dev}, device_id_type=MESH)

    def start_near(self, c):
        @pl.when(self.near_at == 0)
        def _():
            self.rs(self.near, c, self.src.at[self.sl(self.near, c)], self.inward).start()

    def reduce_near(self, c):
        d, sl, src, buf = self.near, self.sl(self.near, c), self.src, self.buf

        @pl.when(self.near_at > 0)
        def _():
            self.rs(d, c, src.at[sl], self.inward).wait_recv()
            buf[d, c] = buf[d, c] + src[sl]
            self.rs(d, c, buf.at[d, c], self.inward).start()

    def reduce_far(self, c):
        d, sl, src, buf = self.far, self.sl(self.far, c), self.src, self.buf

        @pl.when(self.near_at > 0)
        def _():
            self.rs(d, c, src.at[sl], self.outward).wait_recv()
            buf[d, c] = buf[d, c] + src[sl]
            self.rs(d, c, buf.at[d, c], self.outward).start()

    def finish_far(self, c):
        d, sl, src, buf = self.far, self.sl(self.far, c), self.src, self.buf

        @pl.when(self.near_at == 0)
        def _():
            self.rs(d, c, src.at[sl], self.outward).wait_recv()
            self.out[sl] = (self.residual[sl].astype(jnp.float32) + (buf[d, c] + src[sl])).astype(jnp.bfloat16)
            self.bc(d, c, self.inward).start()
            self.ready(d, c)

    def spread_far(self, c):
        @pl.when(self.near_at > 0)
        def _():
            self.bc(self.far, c, self.inward).wait_recv()
            self.bc(self.far, c, self.inward).start()
            self.ready(self.far, c)

    def spread_near(self, c):
        @pl.when(self.near_at > 0)
        def _():
            self.bc(self.near, c, self.outward).wait_recv()
            self.bc(self.near, c, self.outward).start()
            self.ready(self.near, c)

    def finish_near(self, c):
        @pl.when(self.near_at == 0)
        def _():
            self.bc(self.near, c, self.outward).wait_recv()
            self.ready(self.near, c)

    def drain(self, c):
        self.rs(self.near, c, self.src.at[self.sl(self.near, c)], self.inward).wait_send()
        self.bc(self.far, c, self.inward).wait_send()

        @pl.when(self.near_at > 0)
        def _():
            self.rs(self.far, c, self.src.at[self.sl(self.far, c)], self.outward).wait_send()
            self.bc(self.near, c, self.outward).wait_send()

    def stage(self, t, lags=LAGS):
        for fn, lag in ((self.start_near, 0), (self.reduce_near, lags[5]), (self.reduce_far, lags[0]), (self.finish_far, lags[1]), (self.spread_far, lags[2]), (self.spread_near, lags[3]), (self.finish_near, lags[4])):
            if 0 <= t - lag < self.chunks:
                fn(t - lag)

    def run(self):
        for t in range(self.chunks + max(LAGS)):
            self.stage(t)
        for c in range(self.chunks):
            self.drain(c)


def line_scratch(rows, tail, chunks=CHUNKS):
    return [VMEM((2, chunks, rows // (2 * chunks)) + tail, jnp.float32)] + [DMA((2, chunks)) for _ in range(4)]


def norm_rows(src, gain, dst, step=32):
    for r in range(0, src.shape[0], step):
        dst[r:r + step, :] = rms_norm(src[r:r + step, :], gain[...])


def fdot_t(a, b):
    return lax.dot_general(a, b, (((1,), (1,)), ((), ())), preferred_element_type=jnp.float32)


def mlp_act(x, gate, up, act, block):
    def body(j, carry):
        js = pl.ds(pl.multiple_of(j * block, 16), block)
        g = fdot_t(gate[js, :], x[...])
        u = fdot_t(up[js, :], x[...])
        act[js, :] = (g * jax.nn.sigmoid(g) * u).astype(jnp.bfloat16)
        return carry

    lax.fori_loop(0, gate.shape[0] // block, body, 0)


def mlp_down(act, act_t, down, put):
    act_t[...] = act[...].T

    def body(j, carry):
        ns = pl.ds(pl.multiple_of(j * 512, 512), 512)
        put(ns, fdot(act_t[...], down[:, ns]))
        return carry

    lax.fori_loop(0, down.shape[1] // 512, body, 0)


def load(pairs, sem):
    copies = []
    for k, (src, dst) in enumerate(pairs):
        cp = pltpu.make_async_copy(src, dst, sem.at[k])
        cp.start()
        copies.append(cp)
    return copies


def dense_kernel(part, res, gain, ids, w_gate, w_up, w_down, h_out, ids_out, y, x, gate, up, down, act, act_t, part2, id_s, id_r, w_sem, *line):
    z, e = lax.axis_index("tp"), lax.axis_index("ep")
    ends = lax.axis_size("tp") - 1
    width = gate.shape[0]
    loads = load([(w_gate, gate), (w_up, up), (w_down, down)], w_sem)
    n_ep = lax.axis_size("ep")
    peers = [{"ep": lax.rem(e + k, n_ep)} for k in range(1, n_ep)]
    barrier(z, ends, peers)
    sends = []
    for k, dev in enumerate(peers):
        cp = pltpu.make_async_remote_copy(src_ref=ids, dst_ref=ids_out.at[e], send_sem=id_s.at[k], recv_sem=id_r.at[k], device_id=dev, device_id_type=MESH)
        cp.start()
        sends.append(cp)
    ids_out[e] = ids[...]
    one = Line(z, ends, CHUNKS, part, line[0], y, res, line[1:5])

    def normed(d, c):
        x[one.sl(d, c)] = rms_norm(y[one.sl(d, c)], gain[0:1, :])

    one.ready = normed
    one.run()
    loads[0].wait()
    loads[1].wait()
    mlp_act(x, gate, up, act, width // 3)
    loads[2].wait()

    def put(ns, v):
        part2[:, ns] = v

    mlp_down(act, act_t, down, put)
    two = Line(z, ends, CHUNKS, part2, line[5], h_out, y, line[6:10])
    two.run()
    for cp in sends:
        cp.wait()


def dense_block(part, res, gain, ids, w_gate, w_up, w_down):
    rows, hidden = part.shape
    width = w_gate.shape[0]
    vm = pl.BlockSpec(memory_space=VMEM)
    hbm = pl.BlockSpec(memory_space=pl.ANY)
    bf = lambda *s: jax.ShapeDtypeStruct(s, jnp.bfloat16)
    line = line_scratch(rows, (hidden,))
    return pl.pallas_call(
        dense_kernel,
        out_shape=(bf(rows, hidden), jax.ShapeDtypeStruct((4,) + ids.shape, jnp.int32)),
        in_specs=[vm] * 4 + [hbm] * 3,
        out_specs=(vm, vm),
        scratch_shapes=[VMEM((rows, hidden), jnp.bfloat16), VMEM((rows, hidden), jnp.bfloat16), VMEM((width, hidden), jnp.bfloat16), VMEM((width, hidden), jnp.bfloat16), VMEM((width, hidden), jnp.bfloat16), VMEM((width, rows), jnp.bfloat16), VMEM((rows, width), jnp.bfloat16), VMEM((rows, hidden), jnp.float32), DMA((3,)), DMA((3,)), DMA((3,))] + line + line,
        compiler_params=pltpu.CompilerParams(collective_id=1, has_side_effects=True, vmem_limit_bytes=VMEM_CAP),
        name="dense",
    )(part, res, gain, ids, w_gate, w_up, w_down)


def gather_kernel(part, res, gain, router, w_gate, w_up, w_down, y, x_all, shared, probs, p_s, gate, up, down, act, act_t, w_sem, c_s, c_r, y_s, y_r, f_s, f_r, *line):
    z, e = lax.axis_index("tp"), lax.axis_index("ep")
    ends = lax.axis_size("tp") - 1
    width = gate.shape[0]
    rows, hidden = y.shape
    loads = load([(w_gate, gate), (w_up, up), (w_down, down)], w_sem)
    core, chip = jnp.bitwise_xor(e, 1), jnp.bitwise_xor(e, 2)
    barrier(z, ends, [{"ep": core}, {"ep": chip}])
    one = Line(z, ends, CHUNKS, part, line[0], y, res, line[1:5])
    mine = x_all.at[e]

    def copy(src, dst, ss, rs, dev):
        return pltpu.make_async_remote_copy(src_ref=src, dst_ref=dst, send_sem=ss, recv_sem=rs, device_id={"ep": dev}, device_id_type=MESH)

    def to_chip(d, c):
        ref = x_all.at[e, one.sl(d, c)]
        return copy(ref, ref, y_s.at[d, c], y_r.at[d, c], chip)

    def to_core(d, c):
        ref = x_all.at[chip, one.sl(d, c)]
        return copy(ref, ref, f_s.at[d, c], f_r.at[d, c], core)

    def normed(d, c):
        x_all[e, one.sl(d, c)] = rms_norm(y[one.sl(d, c)], gain[1:2, :])
        to_chip(d, c).start()

    one.ready = normed
    one.run()
    own = copy(mine, mine, c_s, c_r, core)
    own.start()
    loads[0].wait()
    loads[1].wait()
    mlp_act(mine, gate, up, act, width // 2)
    loads[2].wait()

    def put(ns, v):
        for j in range(4):
            shared[:, ns.start // 128 + j, :] = v[:, j * 128:(j + 1) * 128]

    mlp_down(act, act_t, down, put)
    def route(j):
        logits = fdot_t(router[...], x_all[j])
        e_x = jnp.exp(logits - jnp.max(logits, axis=0, keepdims=True))
        p_s[...] = e_x / jnp.sum(e_x, axis=0, keepdims=True)
        local = probs.shape[0]
        probs[:, pl.ds(pl.multiple_of(j * rows, rows), rows)] = p_s[pl.ds(pl.multiple_of(e * local, local), local), :]

    route(e)
    every = [(d, c) for c in range(CHUNKS) for d in range(2)]
    for d, c in every:
        to_chip(d, c).wait_recv()
        to_core(d, c).start()
    route(chip)
    own.wait()
    route(core)
    for d, c in every:
        to_chip(d, c).wait_send()
        to_core(d, c).wait()
    route(jnp.bitwise_xor(e, 3))


def gather_block(part, res, gain, router, w_gate, w_up, w_down):
    rows, hidden = part.shape
    width = w_gate.shape[0]
    vm = pl.BlockSpec(memory_space=VMEM)
    hbm = pl.BlockSpec(memory_space=pl.ANY)
    return pl.pallas_call(
        gather_kernel,
        out_shape=(jax.ShapeDtypeStruct((rows, hidden), jnp.bfloat16), jax.ShapeDtypeStruct((4, rows, hidden), jnp.bfloat16), jax.ShapeDtypeStruct((rows, hidden // 128, 128), jnp.float32), jax.ShapeDtypeStruct((router.shape[0] // 4, 4 * rows), jnp.float32)),
        in_specs=[vm] * 4 + [hbm] * 3,
        out_specs=(vm, vm, vm, vm),
        scratch_shapes=[VMEM((router.shape[0], rows), jnp.float32), VMEM((width, hidden), jnp.bfloat16), VMEM((width, hidden), jnp.bfloat16), VMEM((width, hidden), jnp.bfloat16), VMEM((width, rows), jnp.bfloat16), VMEM((rows, width), jnp.bfloat16), DMA((3,)), DMA, DMA] + [DMA((2, CHUNKS)) for _ in range(4)] + line_scratch(rows, (hidden,)),
        compiler_params=pltpu.CompilerParams(collective_id=2, has_side_effects=True, vmem_limit_bytes=VMEM_CAP),
        name="gather",
    )(part, res, gain, router, w_gate, w_up, w_down)


def expert_kernel(own, counts, lists, weights, x_all, shared, w_gate, w_up, w_down, acc_s, x3, rows3, xb, d2, d3):
    e = pl.program_id(0)
    tokens, slabs = x3.shape[0], x3.shape[1]
    local = pl.num_programs(0)

    @pl.when(e == 0)
    def _():
        acc_s[...] = jnp.zeros_like(acc_s)
        xb[...] = jnp.zeros_like(xb)
        acc_s[pl.ds(own[0] * shared.shape[0], shared.shape[0])] = shared[...]

        def widen(i, carry):
            r = pl.ds(pl.multiple_of(i * 64, 64), 64)
            for k in range(slabs):
                x3[r, k, :] = x_all[r, k * 128:(k + 1) * 128].astype(jnp.float32)
            return carry

        lax.fori_loop(0, tokens // 64, widen, 0)

    n = counts[e]

    def tile(i, carry):
        first = i * ROW_TILE
        left = jnp.minimum(n - i * ROW_TILE, ROW_TILE)
        groups = (left + GROUP - 1) // GROUP

        def fetch(g, c):
            sl = pl.ds(pl.multiple_of(g * GROUP, GROUP), GROUP)
            for r in range(GROUP):
                rows3[g * GROUP + r] = x3[lists[e, first + g * GROUP + r]]
            for k in range(slabs):
                xb[sl, k * 128:(k + 1) * 128] = rows3[sl, k, :].astype(jnp.bfloat16)
            return c

        lax.fori_loop(0, groups, fetch, 0)
        g = fdot_t(w_gate[0], xb[...])
        u = fdot_t(w_up[0], xb[...])
        act = (g * jax.nn.sigmoid(g) * u).T.astype(jnp.bfloat16)
        for c in range(0, slabs, 4):
            d2[:, c * 128:(c + 4) * 128] = fdot(act, w_down[0, :, c * 128:(c + 4) * 128])

        def scatter(g, c):
            sl = pl.ds(pl.multiple_of(g * GROUP, GROUP), GROUP)
            for k in range(slabs):
                d3[:, k, :] = d2[sl, k * 128:(k + 1) * 128]
            ts = []
            for r in range(GROUP):
                ok = g * GROUP + r < left
                ts.append(jnp.where(ok, lists[e, first + g * GROUP + r], tokens))
            vals = [acc_s[ts[r]] + weights[e, jnp.minimum(ts[r], tokens - 1)] * d3[r] for r in range(GROUP)]
            for r in range(GROUP):
                acc_s[ts[r]] = vals[r]
            return c

        lax.fori_loop(0, groups, scatter, 0)
        return carry

    lax.fori_loop(0, (n + ROW_TILE - 1) // ROW_TILE, tile, 0)


def expert_block(own, counts, lists, weights, x_all, shared, w_gate, w_up, w_down):
    tokens, hidden = x_all.shape
    local, width, _ = w_gate.shape
    slabs = hidden // 128
    sm = pl.BlockSpec(memory_space=pltpu.SMEM)
    vm = pl.BlockSpec(memory_space=VMEM)
    return pl.pallas_call(
        expert_kernel,
        grid=(local,),
        out_shape=jax.ShapeDtypeStruct((tokens + 8, slabs, 128), jnp.float32),
        in_specs=[sm, sm, sm, sm, vm, vm, pl.BlockSpec((1, width, hidden), lambda e: (e, 0, 0)), pl.BlockSpec((1, width, hidden), lambda e: (e, 0, 0)), pl.BlockSpec((1, width, hidden), lambda e: (e, 0, 0))],
        out_specs=vm,
        scratch_shapes=[VMEM((tokens, slabs, 128), jnp.float32), VMEM((ROW_TILE, slabs, 128), jnp.float32), VMEM((ROW_TILE, hidden), jnp.bfloat16), VMEM((ROW_TILE, hidden), jnp.float32), VMEM((GROUP, slabs, 128), jnp.float32)],
        compiler_params=pltpu.CompilerParams(dimension_semantics=("arbitrary",), vmem_limit_bytes=VMEM_CAP),
        name="experts",
    )(own, counts, lists, weights, x_all, shared, w_gate, w_up, w_down)


def combine_kernel(acc, res, out, total, from_core, from_chip, own_sum, c_s, c_r, y_s, y_r, *line):
    z, e = lax.axis_index("tp"), lax.axis_index("ep")
    ends = lax.axis_size("tp") - 1
    core, chip = jnp.bitwise_xor(e, 1), jnp.bitwise_xor(e, 2)
    both = jnp.bitwise_xor(e, 3)
    barrier(z, ends, [{"ep": core}, {"ep": chip}])
    rows, slabs = res.shape[0], acc.shape[1]
    step = rows // (2 * COMBINE_CHUNKS)
    order = [(d, c) for c in range(COMBINE_CHUNKS) for d in range(2)]

    def copy(src, dst, ss, rs, dev):
        return pltpu.make_async_remote_copy(src_ref=src, dst_ref=dst, send_sem=ss, recv_sem=rs, device_id={"ep": dev}, device_id_type=MESH)

    hops = []
    for w, block in enumerate((both, core)):
        for d, c in order:
            k = d * COMBINE_CHUNKS + c
            cp = copy(acc.at[pl.ds(block * rows + k * step, step)], from_core.at[w, pl.ds(k * step, step)], c_s.at[w, k], c_r.at[w, k], core)
            cp.start()
            hops.append(cp)
    n = len(order)
    outs = []
    for j, (d, c) in enumerate(order):
        k = d * COMBINE_CHUNKS + c
        hops[j].wait_recv()
        sl = pl.ds(k * step, step)
        total[sl] = acc[pl.ds(chip * rows + k * step, step)] + from_core[0, sl]
        cp = copy(total.at[sl], from_chip.at[sl], y_s.at[k], y_r.at[k], chip)
        cp.start()
        outs.append(cp)
    one = Line(z, ends, COMBINE_CHUNKS, own_sum, line[0], out, res, line[1:5])
    for t in range(COMBINE_CHUNKS + max(COMBINE_LAGS)):
        for j in (2 * t, 2 * t + 1):
            if j < n:
                d, c = order[j]
                sl = pl.ds((d * COMBINE_CHUNKS + c) * step, step)
                hops[n + j].wait_recv()
                outs[j].wait_recv()
                from_chip[sl] = (acc[pl.ds(e * rows + (d * COMBINE_CHUNKS + c) * step, step)] + from_core[1, sl]) + from_chip[sl]
                for k in range(slabs):
                    own_sum[sl, k * 128:(k + 1) * 128] = from_chip[sl, k, :]
        one.stage(t, COMBINE_LAGS)
    for c in range(COMBINE_CHUNKS):
        one.drain(c)
    for cp in hops + outs:
        cp.wait_send()


def combine_block(acc, res):
    rows, hidden = res.shape
    slabs, lanes = acc.shape[1:]
    vm = pl.BlockSpec(memory_space=VMEM)
    f32 = lambda *s: VMEM(s, jnp.float32)
    n = 2 * COMBINE_CHUNKS
    return pl.pallas_call(
        combine_kernel,
        out_shape=jax.ShapeDtypeStruct(res.shape, jnp.bfloat16),
        in_specs=[vm, vm],
        out_specs=vm,
        scratch_shapes=[f32(rows, slabs, lanes), f32(2, rows, slabs, lanes), f32(rows, slabs, lanes), f32(rows, hidden), DMA((2, n)), DMA((2, n)), DMA((n,)), DMA((n,))] + line_scratch(rows, (hidden,), COMBINE_CHUNKS),
        compiler_params=pltpu.CompilerParams(collective_id=3, has_side_effects=True, vmem_limit_bytes=VMEM_CAP),
        name="combine",
    )(acc, res)


def token_lists(ids, ep, local):
    tokens = ids.shape[0]
    mine = jnp.any(ids[:, :, None] == (ep * local + jnp.arange(local))[None, None, :], axis=1)
    lower = (jnp.arange(tokens)[:, None] > jnp.arange(tokens)[None, :]).astype(jnp.bfloat16)
    rank = fdot(lower, mine.astype(jnp.bfloat16)).astype(jnp.int32)
    rank = jnp.where(mine, rank, -1)
    hit = rank.T[:, None, :] == jnp.arange(tokens)[None, :, None]
    lists = jnp.sum(jnp.where(hit, jnp.arange(tokens)[None, None, :], 0), axis=2)
    counts = jnp.sum(mine.astype(jnp.int32), axis=0)
    return lists.astype(jnp.int32), counts


def solution(mesh):
    tok_axes = ('dp', 'ep')

    def device_fn(emb, pos, route_ids, lat_cache, rope_cache, attn_norm, w_q, w_dkv, kv_norm, w_uk, w_uv, w_o, mlp_norm, dense_gate, dense_up, dense_down, router, shared_gate, shared_up, shared_down, expert_gate, expert_up, expert_down):
        _, seqs, hidden = emb.shape
        rows = 2 * seqs
        ep = lax.axis_index('ep')
        n_ep = lax.axis_size('ep')
        local = expert_gate.shape[0]
        top_k = route_ids.shape[2]
        cur = jnp.concatenate([pos, pos + 1])
        cos_t, sin_t = rope_tables(cur, rope_cache.shape[-1])
        h0 = emb.reshape(rows, hidden)
        weights = (w_q.transpose(0, 2, 3, 1), w_dkv.swapaxes(1, 2), w_uk, w_uv, w_o, lat_cache, rope_cache)
        attn = lambda layer, h, prev: attn_block(layer, pos, h, attn_norm, kv_norm, cos_t.T, sin_t.T, *weights, prev)
        part, caches = attn(0, h0, None)
        flat = route_ids.reshape(-1)
        ids = jnp.pad(flat, (0, -flat.size % 1024)).reshape(-1, 128)
        h_mid, ids_all = dense_block(part, h0, mlp_norm, ids, dense_gate.T, dense_up.T, dense_down)
        ids_all = ids_all.reshape(n_ep, -1)[:, :flat.size].reshape(n_ep * rows, top_k)
        lists, counts = token_lists(ids_all, ep, local)
        part, caches = attn(1, h_mid, caches)
        y, x_all, shared, probs = gather_block(part, h_mid, mlp_norm, router.T, shared_gate.T, shared_up.T, shared_down)
        x_all = x_all.reshape(n_ep * rows, hidden)
        acc = expert_block(ep.reshape(1), counts, lists, probs, x_all, shared, expert_gate.swapaxes(1, 2), expert_up.swapaxes(1, 2), expert_down)
        out = combine_block(acc, y)
        return out.reshape(2, seqs, hidden), caches[0], caches[1]

    in_specs = (P(None, tok_axes, None), P(tok_axes), P(None, tok_axes, None), P(None, tok_axes, None, None), P(None, tok_axes, None, None), P(), P(None, None, 'tp', None), P(), P(), P(None, None, 'tp', None), P(None, None, 'tp', None), P(None, 'tp', None), P(), P(None, 'tp'), P(None, 'tp'), P('tp', None), P(), P(None, 'tp'), P(None, 'tp'), P('tp', None), P('ep', None, 'tp'), P('ep', None, 'tp'), P('ep', 'tp', None))
    out_specs = (P(None, tok_axes, None), P(None, tok_axes, None, None), P(None, tok_axes, None, None))
    return jax.shard_map(device_fn, mesh=mesh, in_specs=in_specs, out_specs=out_specs, check_vma=False)
```

```python
import functools
import math
import jax
import jax.numpy as jnp
from jax import lax
from jax.experimental import pallas as pl
from jax.experimental.pallas import tpu as pltpu
from jax.sharding import PartitionSpec as P

NORM_EPS = 1e-6
ROPE_THETA = 10000.0
MESH = pl.DeviceIdType.MESH
VMEM = pltpu.VMEM
DMA = pltpu.SemaphoreType.DMA
VMEM_CAP = 62 * 1024 * 1024
SEQ_BLOCK = 16
SEQ_GROUP = 16
CHUNKS = 8
LAGS = (2, 8, 7, 9, 18, 0)
COMBINE_CHUNKS = 8
COMBINE_LAGS = (2, 6, 7, 9, 18, 1)
ROW_TILE = 128
GROUP = 16


def rms_norm(values, gain):
    wide = values.astype(jnp.float32)
    mean_sq = jnp.mean(wide * wide, axis=-1, keepdims=True)
    return (wide * lax.rsqrt(mean_sq + NORM_EPS) * gain).astype(jnp.bfloat16)


def rope_tables(position, rope_dim):
    half_dim = rope_dim // 2
    inv_freq = ROPE_THETA ** (-(jnp.arange(half_dim, dtype=jnp.float32) * 2.0 / rope_dim))
    angles = position.astype(jnp.float32)[:, None] * inv_freq[None, :]
    return jnp.cos(angles), jnp.sin(angles)


def fdot(a, b):
    return jnp.dot(a, b, preferred_element_type=jnp.float32)


def rotate_t(v, cos, sin):
    half = v.shape[0] // 2
    first, second = v[:half], v[half:]
    return jnp.concatenate([first * cos - second * sin, second * cos + first * sin], axis=0)


def rounded(v):
    return v.astype(jnp.bfloat16).astype(jnp.float32)


def attn_kernel(layer, scale, pos_smem, h, gain, kv_gain, cos, sin, w_q, w_kv, w_uk, w_uv, w_o, lat_in, rope_in, *rest):
    lat_out, rope_out, part, x, q_s, qp_s, ln_s, rn_s, o_s = rest[-9:]
    step_id = pl.program_id(0)
    heads, qk = w_q.shape[1], w_q.shape[2]
    seqs, queries, lora = q_s.shape
    rope = rope_in.shape[3]
    nope = qk - rope

    @pl.when(step_id == 0)
    def _():
        norm_rows(h, gain.at[layer:layer + 1], x)
        kv = fdot_t(w_kv[0], x[...])
        lat = kv[:lora]
        lat = lat * lax.rsqrt(jnp.mean(lat * lat, axis=0, keepdims=True) + NORM_EPS)
        ln_s[...] = rounded(lat.T * kv_gain[layer:layer + 1, :])
        rn_s[...] = rounded(rotate_t(kv[lora:], cos[...], sin[...])).T
        for n in range(heads):
            q = fdot_t(w_q[0, n], x[...])
            q_nope = q[:nope].T.astype(jnp.bfloat16)
            q_pe = rotate_t(q[nope:], cos[...], sin[...]).T
            q_lat = fdot_t(q_nope, w_uk[0, :, n, :])
            for s in range(2):
                q_s[:, s * heads + n, :] = q_lat[s * seqs:(s + 1) * seqs]
                qp_s[:, s * heads + n, :] = q_pe[s * seqs:(s + 1) * seqs]

    base = step_id * SEQ_BLOCK
    slots = lat_in.shape[2]
    row_l = lax.broadcasted_iota(jnp.int32, (slots, lora), 0)
    row_r = lax.broadcasted_iota(jnp.int32, (slots, rope), 0)
    step = (lax.broadcasted_iota(jnp.int32, (queries, slots), 0) >= heads).astype(jnp.int32)
    slot = lax.broadcasted_iota(jnp.int32, (queries, slots), 1)
    for first in range(0, SEQ_BLOCK, SEQ_GROUP):
        group = range(first, first + SEQ_GROUP)
        lats, scores = {}, {}
        for i in group:
            p = pos_smem[base + i]
            lat = lat_in[0, i].astype(jnp.float32)
            rop = rope_in[0, i].astype(jnp.float32)
            for s in range(2):
                lat = jnp.where(row_l == p + s, ln_s[pl.ds(s * seqs + base + i, 1), :], lat)
                rop = jnp.where(row_r == p + s, rn_s[pl.ds(s * seqs + base + i, 1), :], rop)
            lats[i] = lat.astype(jnp.bfloat16)
            rop = rop.astype(jnp.bfloat16)
            lat_out[0, i] = lats[i]
            rope_out[0, i] = rop
            sc = fdot_t(q_s[base + i].astype(jnp.bfloat16), lats[i]) + fdot_t(qp_s[base + i].astype(jnp.bfloat16), rop)
            scores[i] = jnp.where(slot <= p + step, sc * scale, -1e30)
        peaks = {i: jnp.max(scores[i], axis=-1, keepdims=True) for i in group}
        exps = {i: jnp.exp(scores[i] - peaks[i]) for i in group}
        sums = {i: jnp.sum(exps[i], axis=-1, keepdims=True) for i in group}
        for i in group:
            o_s[base + i] = fdot((exps[i] / sums[i]).astype(jnp.bfloat16), lats[i])

    @pl.when(step_id == pl.num_programs(0) - 1)
    def _():
        outs = []
        for n in range(heads):
            o = jnp.concatenate([o_s[:, n, :], o_s[:, heads + n, :]], axis=0).astype(jnp.bfloat16)
            outs.append(fdot(o, w_uv[0, :, n, :]).astype(jnp.bfloat16))
        o = jnp.concatenate(outs, axis=1)
        for c in range(0, w_o.shape[2], 512):
            part[:, c:c + 512] = fdot(o, w_o[0, :, c:c + 512])


def attn_block(layer, pos, h, gain, kv_gain, cos, sin, w_q, w_kv, w_uk, w_uv, w_o, lat_cache, rope_cache, prev):
    _, seqs, slots, lora = lat_cache.shape
    rope = rope_cache.shape[3]
    rows, hidden = h.shape
    heads, qk = w_q.shape[1], w_q.shape[2]
    vm = pl.BlockSpec(memory_space=VMEM)
    lay = lambda *tail: pl.BlockSpec((1, SEQ_BLOCK) + tail, lambda i: (layer, i, 0, 0))
    wt = lambda w: pl.BlockSpec((1,) + w.shape[1:], lambda i: (layer,) + (0,) * (w.ndim - 1), pipeline_mode=pl.Buffered(1))
    weights = [w_q, w_kv, w_uk, w_uv, w_o]
    in_specs = [pl.BlockSpec(memory_space=pltpu.SMEM)] + [vm] * 5 + [wt(w) for w in weights] + [lay(slots, lora), lay(slots, rope)]
    args = [pos, h, gain, kv_gain, cos, sin] + weights + [lat_cache, rope_cache]
    alias = {}
    if prev is not None:
        alias = {len(args): 0, len(args) + 1: 1}
        in_specs += [pl.BlockSpec(memory_space=pl.ANY)] * 2
        args += list(prev)
    f32 = lambda *s: VMEM(s, jnp.float32)
    lat, rop, part = pl.pallas_call(
        functools.partial(attn_kernel, layer, 1.0 / math.sqrt(qk)),
        grid=(seqs // SEQ_BLOCK,),
        out_shape=(jax.ShapeDtypeStruct(lat_cache.shape, jnp.bfloat16), jax.ShapeDtypeStruct(rope_cache.shape, jnp.bfloat16), jax.ShapeDtypeStruct((rows, hidden), jnp.float32)),
        in_specs=in_specs,
        out_specs=(lay(slots, lora), lay(slots, rope), vm),
        scratch_shapes=[VMEM((rows, hidden), jnp.bfloat16), f32(seqs, 2 * heads, lora), f32(seqs, 2 * heads, rope), f32(rows, lora), f32(rows, rope), f32(seqs, 2 * heads, lora)],
        input_output_aliases=alias,
        compiler_params=pltpu.CompilerParams(dimension_semantics=("arbitrary",), vmem_limit_bytes=VMEM_CAP),
        name=f"attn{layer}",
    )(*args)
    return part, (lat, rop)


def barrier(z, ends, extra):
    sem = pltpu.get_barrier_semaphore()

    @pl.when(z > 0)
    def _():
        pl.semaphore_signal(sem, inc=1, device_id={"tp": z - 1}, device_id_type=MESH)

    @pl.when(z < ends)
    def _():
        pl.semaphore_signal(sem, inc=1, device_id={"tp": z + 1}, device_id_type=MESH)

    for dev in extra:
        pl.semaphore_signal(sem, inc=1, device_id=dev, device_id_type=MESH)
    count = len(extra) + jnp.where(z > 0, 1, 0) + jnp.where(z < ends, 1, 0)
    pl.semaphore_wait(sem, count)


class Line:
    def __init__(self, z, ends, chunks, src, buf, out, residual, sems):
        self.z, self.ends, self.chunks = z, ends, chunks
        self.src, self.buf, self.out, self.residual = src, buf, out, residual
        self.rs_s, self.rs_r, self.bc_s, self.bc_r = sems
        self.rows = src.shape[0] // (2 * chunks)
        low = 2 * z < ends
        self.near = jnp.where(low, 1, 0)
        self.far = 1 - self.near
        self.near_at = jnp.where(low, z, ends - z)
        self.far_at = ends - self.near_at
        up, down = jnp.minimum(z + 1, ends), jnp.maximum(z - 1, 0)
        self.inward = jnp.where(low, up, down)
        self.outward = jnp.where(low, down, up)

    def ready(self, d, c):
        pass

    def sl(self, d, c):
        return pl.ds(pl.multiple_of((d * self.chunks + c) * self.rows, self.rows), self.rows)

    def rs(self, d, c, src, dev):
        return pltpu.make_async_remote_copy(src_ref=src, dst_ref=self.buf.at[d, c], send_sem=self.rs_s.at[d, c], recv_sem=self.rs_r.at[d, c], device_id={"tp": dev}, device_id_type=MESH)

    def bc(self, d, c, dev):
        ref = self.out.at[self.sl(d, c)]
        return pltpu.make_async_remote_copy(src_ref=ref, dst_ref=ref, send_sem=self.bc_s.at[d, c], recv_sem=self.bc_r.at[d, c], device_id={"tp": dev}, device_id_type=MESH)

    def start_near(self, c):
        @pl.when(self.near_at == 0)
        def _():
            self.rs(self.near, c, self.src.at[self.sl(self.near, c)], self.inward).start()

    def reduce_near(self, c):
        d, sl, src, buf = self.near, self.sl(self.near, c), self.src, self.buf

        @pl.when(self.near_at > 0)
        def _():
            self.rs(d, c, src.at[sl], self.inward).wait_recv()
            buf[d, c] = buf[d, c] + src[sl]
            self.rs(d, c, buf.at[d, c], self.inward).start()

    def reduce_far(self, c):
        d, sl, src, buf = self.far, self.sl(self.far, c), self.src, self.buf

        @pl.when(self.near_at > 0)
        def _():
            self.rs(d, c, src.at[sl], self.outward).wait_recv()
            buf[d, c] = buf[d, c] + src[sl]
            self.rs(d, c, buf.at[d, c], self.outward).start()

    def finish_far(self, c):
        d, sl, src, buf = self.far, self.sl(self.far, c), self.src, self.buf

        @pl.when(self.near_at == 0)
        def _():
            self.rs(d, c, src.at[sl], self.outward).wait_recv()
            self.out[sl] = (self.residual[sl].astype(jnp.float32) + (buf[d, c] + src[sl])).astype(jnp.bfloat16)
            self.bc(d, c, self.inward).start()
            self.ready(d, c)

    def spread_far(self, c):
        @pl.when(self.near_at > 0)
        def _():
            self.bc(self.far, c, self.inward).wait_recv()
            self.bc(self.far, c, self.inward).start()
            self.ready(self.far, c)

    def spread_near(self, c):
        @pl.when(self.near_at > 0)
        def _():
            self.bc(self.near, c, self.outward).wait_recv()
            self.bc(self.near, c, self.outward).start()
            self.ready(self.near, c)

    def finish_near(self, c):
        @pl.when(self.near_at == 0)
        def _():
            self.bc(self.near, c, self.outward).wait_recv()
            self.ready(self.near, c)

    def drain(self, c):
        self.rs(self.near, c, self.src.at[self.sl(self.near, c)], self.inward).wait_send()
        self.bc(self.far, c, self.inward).wait_send()

        @pl.when(self.near_at > 0)
        def _():
            self.rs(self.far, c, self.src.at[self.sl(self.far, c)], self.outward).wait_send()
            self.bc(self.near, c, self.outward).wait_send()

    def stage(self, t, lags=LAGS):
        for fn, lag in ((self.start_near, 0), (self.reduce_near, lags[5]), (self.reduce_far, lags[0]), (self.finish_far, lags[1]), (self.spread_far, lags[2]), (self.spread_near, lags[3]), (self.finish_near, lags[4])):
            if 0 <= t - lag < self.chunks:
                fn(t - lag)

    def run(self):
        for t in range(self.chunks + max(LAGS)):
            self.stage(t)
        for c in range(self.chunks):
            self.drain(c)


def line_scratch(rows, tail, chunks=CHUNKS):
    return [VMEM((2, chunks, rows // (2 * chunks)) + tail, jnp.float32)] + [DMA((2, chunks)) for _ in range(4)]


def norm_rows(src, gain, dst, step=32):
    for r in range(0, src.shape[0], step):
        dst[r:r + step, :] = rms_norm(src[r:r + step, :], gain[...])


def fdot_t(a, b):
    return lax.dot_general(a, b, (((1,), (1,)), ((), ())), preferred_element_type=jnp.float32)


def mlp_act(x, gate, up, act, block):
    def body(j, carry):
        js = pl.ds(pl.multiple_of(j * block, 16), block)
        g = fdot_t(gate[js, :], x[...])
        u = fdot_t(up[js, :], x[...])
        act[js, :] = (g * jax.nn.sigmoid(g) * u).astype(jnp.bfloat16)
        return carry

    lax.fori_loop(0, gate.shape[0] // block, body, 0)


def mlp_down(act, act_t, down, put):
    act_t[...] = act[...].T

    def body(j, carry):
        ns = pl.ds(pl.multiple_of(j * 512, 512), 512)
        put(ns, fdot(act_t[...], down[:, ns]))
        return carry

    lax.fori_loop(0, down.shape[1] // 512, body, 0)


def load(pairs, sem):
    copies = []
    for k, (src, dst) in enumerate(pairs):
        cp = pltpu.make_async_copy(src, dst, sem.at[k])
        cp.start()
        copies.append(cp)
    return copies


def dense_kernel(part, res, gain, ids, w_gate, w_up, w_down, h_out, ids_out, y, x, gate, up, down, act, act_t, part2, id_s, id_r, w_sem, *line):
    z, e = lax.axis_index("tp"), lax.axis_index("ep")
    ends = lax.axis_size("tp") - 1
    width = gate.shape[0]
    loads = load([(w_gate, gate), (w_up, up), (w_down, down)], w_sem)
    n_ep = lax.axis_size("ep")
    peers = [{"ep": lax.rem(e + k, n_ep)} for k in range(1, n_ep)]
    barrier(z, ends, peers)
    sends = []
    for k, dev in enumerate(peers):
        cp = pltpu.make_async_remote_copy(src_ref=ids, dst_ref=ids_out.at[e], send_sem=id_s.at[k], recv_sem=id_r.at[k], device_id=dev, device_id_type=MESH)
        cp.start()
        sends.append(cp)
    ids_out[e] = ids[...]
    one = Line(z, ends, CHUNKS, part, line[0], y, res, line[1:5])

    def normed(d, c):
        x[one.sl(d, c)] = rms_norm(y[one.sl(d, c)], gain[0:1, :])

    one.ready = normed
    one.run()
    loads[0].wait()
    loads[1].wait()
    mlp_act(x, gate, up, act, width // 3)
    loads[2].wait()

    def put(ns, v):
        part2[:, ns] = v

    mlp_down(act, act_t, down, put)
    two = Line(z, ends, CHUNKS, part2, line[5], h_out, y, line[6:10])
    two.run()
    for cp in sends:
        cp.wait()


def dense_block(part, res, gain, ids, w_gate, w_up, w_down):
    rows, hidden = part.shape
    width = w_gate.shape[0]
    vm = pl.BlockSpec(memory_space=VMEM)
    hbm = pl.BlockSpec(memory_space=pl.ANY)
    bf = lambda *s: jax.ShapeDtypeStruct(s, jnp.bfloat16)
    line = line_scratch(rows, (hidden,))
    return pl.pallas_call(
        dense_kernel,
        out_shape=(bf(rows, hidden), jax.ShapeDtypeStruct((4,) + ids.shape, jnp.int32)),
        in_specs=[vm] * 4 + [hbm] * 3,
        out_specs=(vm, vm),
        scratch_shapes=[VMEM((rows, hidden), jnp.bfloat16), VMEM((rows, hidden), jnp.bfloat16), VMEM((width, hidden), jnp.bfloat16), VMEM((width, hidden), jnp.bfloat16), VMEM((width, hidden), jnp.bfloat16), VMEM((width, rows), jnp.bfloat16), VMEM((rows, width), jnp.bfloat16), VMEM((rows, hidden), jnp.float32), DMA((3,)), DMA((3,)), DMA((3,))] + line + line,
        compiler_params=pltpu.CompilerParams(collective_id=1, has_side_effects=True, vmem_limit_bytes=VMEM_CAP),
        name="dense",
    )(part, res, gain, ids, w_gate, w_up, w_down)


def gather_kernel(part, res, gain, router, w_gate, w_up, w_down, y, x_all, shared, probs, p_s, gate, up, down, act, act_t, w_sem, c_s, c_r, y_s, y_r, f_s, f_r, *line):
    z, e = lax.axis_index("tp"), lax.axis_index("ep")
    ends = lax.axis_size("tp") - 1
    width = gate.shape[0]
    rows, hidden = y.shape
    loads = load([(w_gate, gate), (w_up, up), (w_down, down)], w_sem)
    core, chip = jnp.bitwise_xor(e, 1), jnp.bitwise_xor(e, 2)
    barrier(z, ends, [{"ep": core}, {"ep": chip}])
    one = Line(z, ends, CHUNKS, part, line[0], y, res, line[1:5])
    mine = x_all.at[e]

    def copy(src, dst, ss, rs, dev):
        return pltpu.make_async_remote_copy(src_ref=src, dst_ref=dst, send_sem=ss, recv_sem=rs, device_id={"ep": dev}, device_id_type=MESH)

    def to_chip(d, c):
        ref = x_all.at[e, one.sl(d, c)]
        return copy(ref, ref, y_s.at[d, c], y_r.at[d, c], chip)

    def to_core(d, c):
        ref = x_all.at[chip, one.sl(d, c)]
        return copy(ref, ref, f_s.at[d, c], f_r.at[d, c], core)

    def normed(d, c):
        x_all[e, one.sl(d, c)] = rms_norm(y[one.sl(d, c)], gain[1:2, :])
        to_chip(d, c).start()

    one.ready = normed
    one.run()
    own = copy(mine, mine, c_s, c_r, core)
    own.start()
    loads[0].wait()
    loads[1].wait()
    mlp_act(mine, gate, up, act, width // 2)
    loads[2].wait()

    def put(ns, v):
        for j in range(4):
            shared[:, ns.start // 128 + j, :] = v[:, j * 128:(j + 1) * 128]

    mlp_down(act, act_t, down, put)
    def route(j):
        logits = fdot_t(router[...], x_all[j])
        e_x = jnp.exp(logits - jnp.max(logits, axis=0, keepdims=True))
        p_s[...] = e_x / jnp.sum(e_x, axis=0, keepdims=True)
        local = probs.shape[0]
        probs[:, pl.ds(pl.multiple_of(j * rows, rows), rows)] = p_s[pl.ds(pl.multiple_of(e * local, local), local), :]

    route(e)
    every = [(d, c) for c in range(CHUNKS) for d in range(2)]
    for d, c in every:
        to_chip(d, c).wait_recv()
        to_core(d, c).start()
    route(chip)
    own.wait()
    route(core)
    for d, c in every:
        to_chip(d, c).wait_send()
        to_core(d, c).wait()
    route(jnp.bitwise_xor(e, 3))


def gather_block(part, res, gain, router, w_gate, w_up, w_down):
    rows, hidden = part.shape
    width = w_gate.shape[0]
    vm = pl.BlockSpec(memory_space=VMEM)
    hbm = pl.BlockSpec(memory_space=pl.ANY)
    return pl.pallas_call(
        gather_kernel,
        out_shape=(jax.ShapeDtypeStruct((rows, hidden), jnp.bfloat16), jax.ShapeDtypeStruct((4, rows, hidden), jnp.bfloat16), jax.ShapeDtypeStruct((rows, hidden // 128, 128), jnp.float32), jax.ShapeDtypeStruct((router.shape[0] // 4, 4 * rows), jnp.float32)),
        in_specs=[vm] * 4 + [hbm] * 3,
        out_specs=(vm, vm, vm, vm),
        scratch_shapes=[VMEM((router.shape[0], rows), jnp.float32), VMEM((width, hidden), jnp.bfloat16), VMEM((width, hidden), jnp.bfloat16), VMEM((width, hidden), jnp.bfloat16), VMEM((width, rows), jnp.bfloat16), VMEM((rows, width), jnp.bfloat16), DMA((3,)), DMA, DMA] + [DMA((2, CHUNKS)) for _ in range(4)] + line_scratch(rows, (hidden,)),
        compiler_params=pltpu.CompilerParams(collective_id=2, has_side_effects=True, vmem_limit_bytes=VMEM_CAP),
        name="gather",
    )(part, res, gain, router, w_gate, w_up, w_down)


def expert_kernel(own, counts, lists, weights, x_all, shared, w_gate, w_up, w_down, acc_s, x3, rows3, xb, d2, d3):
    e = pl.program_id(0)
    tokens, slabs = x3.shape[0], x3.shape[1]
    local = pl.num_programs(0)

    @pl.when(e == 0)
    def _():
        acc_s[...] = jnp.zeros_like(acc_s)
        xb[...] = jnp.zeros_like(xb)
        acc_s[pl.ds(own[0] * shared.shape[0], shared.shape[0])] = shared[...]

        def widen(i, carry):
            r = pl.ds(pl.multiple_of(i * 64, 64), 64)
            for k in range(slabs):
                x3[r, k, :] = x_all[r, k * 128:(k + 1) * 128].astype(jnp.float32)
            return carry

        lax.fori_loop(0, tokens // 64, widen, 0)

    n = counts[e]

    def tile(i, carry):
        first = i * ROW_TILE
        left = jnp.minimum(n - i * ROW_TILE, ROW_TILE)
        groups = (left + GROUP - 1) // GROUP

        def fetch(g, c):
            sl = pl.ds(pl.multiple_of(g * GROUP, GROUP), GROUP)
            for r in range(GROUP):
                rows3[g * GROUP + r] = x3[lists[e, first + g * GROUP + r]]
            for k in range(slabs):
                xb[sl, k * 128:(k + 1) * 128] = rows3[sl, k, :].astype(jnp.bfloat16)
            return c

        lax.fori_loop(0, groups, fetch, 0)
        g = fdot_t(w_gate[0], xb[...])
        u = fdot_t(w_up[0], xb[...])
        act = (g * jax.nn.sigmoid(g) * u).T.astype(jnp.bfloat16)
        for c in range(0, slabs, 4):
            d2[:, c * 128:(c + 4) * 128] = fdot(act, w_down[0, :, c * 128:(c + 4) * 128])

        def scatter(g, c):
            sl = pl.ds(pl.multiple_of(g * GROUP, GROUP), GROUP)
            for k in range(slabs):
                d3[:, k, :] = d2[sl, k * 128:(k + 1) * 128]
            ts = []
            for r in range(GROUP):
                ok = g * GROUP + r < left
                ts.append(jnp.where(ok, lists[e, first + g * GROUP + r], tokens))
            vals = [acc_s[ts[r]] + weights[e, jnp.minimum(ts[r], tokens - 1)] * d3[r] for r in range(GROUP)]
            for r in range(GROUP):
                acc_s[ts[r]] = vals[r]
            return c

        lax.fori_loop(0, groups, scatter, 0)
        return carry

    lax.fori_loop(0, (n + ROW_TILE - 1) // ROW_TILE, tile, 0)


def expert_block(own, counts, lists, weights, x_all, shared, w_gate, w_up, w_down):
    tokens, hidden = x_all.shape
    local, width, _ = w_gate.shape
    slabs = hidden // 128
    sm = pl.BlockSpec(memory_space=pltpu.SMEM)
    vm = pl.BlockSpec(memory_space=VMEM)
    return pl.pallas_call(
        expert_kernel,
        grid=(local,),
        out_shape=jax.ShapeDtypeStruct((tokens + 8, slabs, 128), jnp.float32),
        in_specs=[sm, sm, sm, sm, vm, vm, pl.BlockSpec((1, width, hidden), lambda e: (e, 0, 0)), pl.BlockSpec((1, width, hidden), lambda e: (e, 0, 0)), pl.BlockSpec((1, width, hidden), lambda e: (e, 0, 0))],
        out_specs=vm,
        scratch_shapes=[VMEM((tokens, slabs, 128), jnp.float32), VMEM((ROW_TILE, slabs, 128), jnp.float32), VMEM((ROW_TILE, hidden), jnp.bfloat16), VMEM((ROW_TILE, hidden), jnp.float32), VMEM((GROUP, slabs, 128), jnp.float32)],
        compiler_params=pltpu.CompilerParams(dimension_semantics=("arbitrary",), vmem_limit_bytes=VMEM_CAP),
        name="experts",
    )(own, counts, lists, weights, x_all, shared, w_gate, w_up, w_down)


def combine_kernel(acc, res, out, total, from_core, from_chip, own_sum, c_s, c_r, y_s, y_r, *line):
    z, e = lax.axis_index("tp"), lax.axis_index("ep")
    ends = lax.axis_size("tp") - 1
    core, chip = jnp.bitwise_xor(e, 1), jnp.bitwise_xor(e, 2)
    both = jnp.bitwise_xor(e, 3)
    barrier(z, ends, [{"ep": core}, {"ep": chip}])
    rows, slabs = res.shape[0], acc.shape[1]
    step = rows // (2 * COMBINE_CHUNKS)
    order = [(d, c) for c in range(COMBINE_CHUNKS) for d in range(2)]

    def copy(src, dst, ss, rs, dev):
        return pltpu.make_async_remote_copy(src_ref=src, dst_ref=dst, send_sem=ss, recv_sem=rs, device_id={"ep": dev}, device_id_type=MESH)

    hops = []
    for w, block in enumerate((both, core)):
        for d, c in order:
            k = d * COMBINE_CHUNKS + c
            cp = copy(acc.at[pl.ds(block * rows + k * step, step)], from_core.at[w, pl.ds(k * step, step)], c_s.at[w, k], c_r.at[w, k], core)
            cp.start()
            hops.append(cp)
    n = len(order)
    outs = []
    for j, (d, c) in enumerate(order):
        k = d * COMBINE_CHUNKS + c
        hops[j].wait_recv()
        sl = pl.ds(k * step, step)
        total[sl] = acc[pl.ds(chip * rows + k * step, step)] + from_core[0, sl]
        cp = copy(total.at[sl], from_chip.at[sl], y_s.at[k], y_r.at[k], chip)
        cp.start()
        outs.append(cp)
    one = Line(z, ends, COMBINE_CHUNKS, own_sum, line[0], out, res, line[1:5])
    for t in range(COMBINE_CHUNKS + max(COMBINE_LAGS)):
        for j in (2 * t, 2 * t + 1):
            if j < n:
                d, c = order[j]
                sl = pl.ds((d * COMBINE_CHUNKS + c) * step, step)
                hops[n + j].wait_recv()
                outs[j].wait_recv()
                from_chip[sl] = (acc[pl.ds(e * rows + (d * COMBINE_CHUNKS + c) * step, step)] + from_core[1, sl]) + from_chip[sl]
                for k in range(slabs):
                    own_sum[sl, k * 128:(k + 1) * 128] = from_chip[sl, k, :]
        one.stage(t, COMBINE_LAGS)
    for c in range(COMBINE_CHUNKS):
        one.drain(c)
    for cp in hops + outs:
        cp.wait_send()


def combine_block(acc, res):
    rows, hidden = res.shape
    slabs, lanes = acc.shape[1:]
    vm = pl.BlockSpec(memory_space=VMEM)
    f32 = lambda *s: VMEM(s, jnp.float32)
    n = 2 * COMBINE_CHUNKS
    return pl.pallas_call(
        combine_kernel,
        out_shape=jax.ShapeDtypeStruct(res.shape, jnp.bfloat16),
        in_specs=[vm, vm],
        out_specs=vm,
        scratch_shapes=[f32(rows, slabs, lanes), f32(2, rows, slabs, lanes), f32(rows, slabs, lanes), f32(rows, hidden), DMA((2, n)), DMA((2, n)), DMA((n,)), DMA((n,))] + line_scratch(rows, (hidden,), COMBINE_CHUNKS),
        compiler_params=pltpu.CompilerParams(collective_id=3, has_side_effects=True, vmem_limit_bytes=VMEM_CAP),
        name="combine",
    )(acc, res)


def token_lists(ids, ep, local):
    tokens = ids.shape[0]
    mine = jnp.any(ids[:, :, None] == (ep * local + jnp.arange(local))[None, None, :], axis=1)
    lower = (jnp.arange(tokens)[:, None] > jnp.arange(tokens)[None, :]).astype(jnp.bfloat16)
    rank = fdot(lower, mine.astype(jnp.bfloat16)).astype(jnp.int32)
    rank = jnp.where(mine, rank, -1)
    token = jnp.arange(tokens)
    lists = jnp.sum(jnp.where(rank[:, :, None] == token[None, None, :], token[:, None, None], 0), axis=0)
    counts = jnp.sum(mine.astype(jnp.int32), axis=0)
    return lists.astype(jnp.int32), counts


def solution(mesh):
    tok_axes = ('dp', 'ep')

    def device_fn(emb, pos, route_ids, lat_cache, rope_cache, attn_norm, w_q, w_dkv, kv_norm, w_uk, w_uv, w_o, mlp_norm, dense_gate, dense_up, dense_down, router, shared_gate, shared_up, shared_down, expert_gate, expert_up, expert_down):
        _, seqs, hidden = emb.shape
        rows = 2 * seqs
        ep = lax.axis_index('ep')
        n_ep = lax.axis_size('ep')
        local = expert_gate.shape[0]
        top_k = route_ids.shape[2]
        cur = jnp.concatenate([pos, pos + 1])
        cos_t, sin_t = rope_tables(cur, rope_cache.shape[-1])
        h0 = emb.reshape(rows, hidden)
        weights = (w_q.transpose(0, 2, 3, 1), w_dkv.swapaxes(1, 2), w_uk, w_uv, w_o, lat_cache, rope_cache)
        attn = lambda layer, h, prev: attn_block(layer, pos, h, attn_norm, kv_norm, cos_t.T, sin_t.T, *weights, prev)
        part, caches = attn(0, h0, None)
        flat = route_ids.reshape(-1)
        ids = jnp.pad(flat, (0, -flat.size % 1024)).reshape(-1, 128)
        h_mid, ids_all = dense_block(part, h0, mlp_norm, ids, dense_gate.T, dense_up.T, dense_down)
        ids_all = ids_all.reshape(n_ep, -1)[:, :flat.size].reshape(n_ep * rows, top_k)
        lists, counts = token_lists(ids_all, ep, local)
        part, caches = attn(1, h_mid, caches)
        y, x_all, shared, probs = gather_block(part, h_mid, mlp_norm, router.T, shared_gate.T, shared_up.T, shared_down)
        x_all = x_all.reshape(n_ep * rows, hidden)
        acc = expert_block(ep.reshape(1), counts, lists, probs, x_all, shared, expert_gate.swapaxes(1, 2), expert_up.swapaxes(1, 2), expert_down)
        out = combine_block(acc, y)
        return out.reshape(2, seqs, hidden), caches[0], caches[1]

    in_specs = (P(None, tok_axes, None), P(tok_axes), P(None, tok_axes, None), P(None, tok_axes, None, None), P(None, tok_axes, None, None), P(), P(None, None, 'tp', None), P(), P(), P(None, None, 'tp', None), P(None, None, 'tp', None), P(None, 'tp', None), P(), P(None, 'tp'), P(None, 'tp'), P('tp', None), P(), P(None, 'tp'), P(None, 'tp'), P('tp', None), P('ep', None, 'tp'), P('ep', None, 'tp'), P('ep', 'tp', None))
    out_specs = (P(None, tok_axes, None), P(None, tok_axes, None, None), P(None, tok_axes, None, None))
    return jax.shard_map(device_fn, mesh=mesh, in_specs=in_specs, out_specs=out_specs, check_vma=False)
```
